256 devices in a mesh: kv: 32 (over z, y_lo, core), batch: 8 (over y_hi, x).
Axes of the slice: x: 4, y: 4 (y_hi: 2, y_lo: 2; y = y_hi * 2 + y_lo), z: 8, core: 2. Of those that a mesh axis runs over, the one named last changes fastest.
Arguments:
- queries: bfloat16 [256, 4, 32, 128], P(('kv', 'batch')), may hold values from -200 to 200
- prefix_keys: bfloat16 [16384, 16, 128], P(('kv', 'batch')), may hold values from -12 to 12
- prefix_values: bfloat16 [16384, 16, 128], P(('kv', 'batch')), may hold values from -12 to 12
- suffix_keys: bfloat16 [256, 1024, 16, 128], P(('kv', 'batch')), may hold values from -14 to 14
- suffix_values: bfloat16 [256, 1024, 16, 128], P(('kv', 'batch')), may hold values from -12 to 12
- lengths: int32 [256], P(('kv', 'batch')), may hold values from 256 to 1024, as said below
Outputs:
- attended: bfloat16 [256, 4, 32, 128], P(('kv', 'batch'))
The draws below stay inside these ranges and needn't reach their ends.
Inputs may be any that keep to these rules, and one draw needn't show every extreme that they name: `lengths`: each sequence's own cache holds its 4 new tokens in its last used slots; some sequence fills all 1024 slots.
All inputs are finite; a program needn't handle non-finite values.
Results may differ from the reference program's by a relative error of at most 0.0045.
Values may be sent and summed in bfloat16 or wider, within the bound.
A program may use at most 64 MiB of HBM per device.

```python
import jax
import jax.numpy as jnp
from jax import lax

QH = 32
KV_HEADS = 16
HEAD_WIDTH = 128
QUERY_SCALE = 144
NEW_QUERY_COUNT = 4
SUFFIX = 1024
PREFIX_DEV = 64
SEQUENCE_COUNT = 256
PREFIX = 16384


def prompt_key_core(key):
    base = jax.random.normal(jax.random.fold_in(key, 101), (PREFIX, KV_HEADS, HEAD_WIDTH), jnp.float32)
    shifts = jax.random.normal(jax.random.fold_in(key, 102), (PREFIX // PREFIX_DEV, KV_HEADS, HEAD_WIDTH), jnp.float32) * 1.5
    return jnp.clip(base + jnp.repeat(shifts, PREFIX_DEV, axis=0), -12.0, 12.0)


def draw_prefix_keys(key, part):
    return prompt_key_core(key).astype(jnp.bfloat16)


def draw_prefix_values(key, part):
    base = jax.random.normal(jax.random.fold_in(key, 111), (PREFIX, KV_HEADS, HEAD_WIDTH), jnp.float32)
    shifts = jax.random.normal(jax.random.fold_in(key, 112), (PREFIX // PREFIX_DEV, KV_HEADS, HEAD_WIDTH), jnp.float32) * 2.0
    return jnp.clip(base + jnp.repeat(shifts, PREFIX_DEV, axis=0), -12.0, 12.0).astype(jnp.bfloat16)


def draw_queries(key, part):
    factor = 1.5
    values = jax.random.normal(jax.random.fold_in(key, 103), (SEQUENCE_COUNT, NEW_QUERY_COUNT, QH, HEAD_WIDTH), jnp.float32)
    values = jnp.clip(values, -6.0, 6.0) * factor
    prompt = prompt_key_core(key).astype(jnp.bfloat16).astype(jnp.float32)
    chosen = jax.random.randint(jax.random.fold_in(key, 104), (6,), 0, SEQUENCE_COUNT)
    first_pos = jax.random.randint(jax.random.fold_in(key, 105), (6,), 0, PREFIX)
    second_pos = jax.random.randint(jax.random.fold_in(key, 106), (6,), 0, PREFIX)
    levels = jnp.array([4.5, 3.0, 1.5, 3.0, 4.5, 1.5], jnp.float32)
    strength = levels * (512.0 / HEAD_WIDTH)
    paired = (prompt[first_pos] + prompt[second_pos]) * 0.5
    paired = jnp.repeat(paired, QH // KV_HEADS, axis=1)
    values = values.at[chosen, 0].set(strength[:, None, None] * paired)
    return jnp.clip(values, -200.0, 200.0).astype(jnp.bfloat16)


def draw_lengths(key, part):
    drawn = jax.random.randint(jax.random.fold_in(key, 107), (SEQUENCE_COUNT,), SUFFIX // 4, SUFFIX + 1)
    fullest = jax.random.randint(jax.random.fold_in(key, 108), (), 0, SEQUENCE_COUNT)
    return drawn.at[fullest].set(SUFFIX).astype(jnp.int32)


def level_of(own_key, dims, pieces, smallest, top_value):
    def one(position, parts):
        draws = jax.random.uniform(jax.random.fold_in(jax.random.fold_in(own_key, 6), position), (parts,), jnp.float32, smallest / len(pieces), top_value / len(pieces))
        return jnp.repeat(jnp.exp(draws), dims[position] // parts).reshape((-1,) + (1,) * (len(dims) - position - 1))

    loudness = one(*pieces[0])
    for cut in pieces[1:]:
        loudness = loudness * one(*cut)
    return loudness


def gaussian(stream_key, extent, width, reach, cuts=(), kind=jnp.bfloat16):
    loudness = level_of(stream_key, extent, cuts, -0.22, 0.18) if cuts else 1.0
    values = jax.random.normal(stream_key, extent, jnp.float32) * width * loudness
    return jnp.minimum(jnp.maximum(values, -reach), reach).astype(kind)


def setup_inputs(seed: int = 0) -> dict:
    arg_keys = jax.random.split(jax.random.key(seed), 7)
    queries = draw_queries(jax.random.fold_in(arg_keys[6], 71), 0)
    prefix_keys = draw_prefix_keys(jax.random.fold_in(arg_keys[6], 71), 0)
    prefix_values = draw_prefix_values(jax.random.fold_in(arg_keys[6], 71), 0)
    suffix_keys = gaussian(arg_keys[3], (SEQUENCE_COUNT, SUFFIX, KV_HEADS, HEAD_WIDTH), 2.5, 14.0, ((0, 256),))
    suffix_values = gaussian(arg_keys[4], (SEQUENCE_COUNT, SUFFIX, KV_HEADS, HEAD_WIDTH), 2.5, 12.0, ((0, 256),))
    lengths = draw_lengths(jax.random.fold_in(arg_keys[6], 71), 0)
    return {"queries": queries, "prefix_keys": prefix_keys, "prefix_values": prefix_values, "suffix_keys": suffix_keys, "suffix_values": suffix_values, "lengths": lengths}


masked_score = -1.0e30


def reference(queries, prefix_keys, prefix_values, suffix_keys, suffix_values, lengths):
    scaling = QUERY_SCALE ** -0.5
    queries_per_group = QH // KV_HEADS
    grouped = queries.reshape(SEQUENCE_COUNT, NEW_QUERY_COUNT, KV_HEADS, queries_per_group, HEAD_WIDTH)
    limits = lengths[:, None] - NEW_QUERY_COUNT + 1 + jnp.arange(NEW_QUERY_COUNT, dtype=jnp.int32)[None, :]
    limits = jnp.repeat(limits, queries_per_group, axis=1)
    positions = jnp.arange(SUFFIX, dtype=jnp.int32)
    visible = positions[None, None, :] < limits[:, :, None]

    def one_head(head):
        query_rows = lax.dynamic_index_in_dim(grouped, head, 2, keepdims=False)
        keys_prompt = lax.dynamic_index_in_dim(prefix_keys, head, 1, keepdims=False)
        values_prompt = lax.dynamic_index_in_dim(prefix_values, head, 1, keepdims=False)
        keys_own = lax.dynamic_index_in_dim(suffix_keys, head, 2, keepdims=False)
        suffix_value_rows = lax.dynamic_index_in_dim(suffix_values, head, 2, keepdims=False)
        flat_rows = query_rows.reshape(SEQUENCE_COUNT * NEW_QUERY_COUNT * queries_per_group, HEAD_WIDTH)
        prompt_scores = jnp.dot(flat_rows, keys_prompt.T, preferred_element_type=jnp.float32) * scaling
        prompt_scores = prompt_scores.reshape(SEQUENCE_COUNT, NEW_QUERY_COUNT * queries_per_group, PREFIX)
        suffix_scores = jnp.einsum("ixv,iav->ixa", query_rows.reshape(SEQUENCE_COUNT, NEW_QUERY_COUNT * queries_per_group, HEAD_WIDTH).astype(jnp.float32),
                                keys_own.astype(jnp.float32)) * scaling
        suffix_scores = jnp.where(visible, suffix_scores, masked_score)
        top = jnp.maximum(jnp.max(prompt_scores, -1), jnp.max(suffix_scores, -1))
        prompt_weights = jnp.exp(prompt_scores - top[..., None])
        own_weights = jnp.exp(suffix_scores - top[..., None])
        total = jnp.sum(prompt_weights, -1) + jnp.sum(own_weights, -1)
        prompt_rounded = prompt_weights.astype(jnp.bfloat16).reshape(SEQUENCE_COUNT * NEW_QUERY_COUNT * queries_per_group, PREFIX)
        prompt_part = jnp.dot(prompt_rounded, values_prompt, preferred_element_type=jnp.float32)
        prompt_part = prompt_part.reshape(SEQUENCE_COUNT, NEW_QUERY_COUNT * queries_per_group, HEAD_WIDTH)
        suffix_rounded = lax.optimization_barrier(own_weights.astype(jnp.bfloat16))
        suffix_partial = jnp.einsum("caj,cjv->cav", suffix_rounded.astype(jnp.float32), suffix_value_rows.astype(jnp.float32))
        result = (prompt_part + suffix_partial) / total[..., None]
        return result.reshape(SEQUENCE_COUNT, NEW_QUERY_COUNT, queries_per_group, HEAD_WIDTH)

    outputs = lax.map(one_head, jnp.arange(KV_HEADS, dtype=jnp.int32))
    outputs = jnp.moveaxis(outputs, 0, 2)
    return outputs.reshape(SEQUENCE_COUNT, NEW_QUERY_COUNT, QH, HEAD_WIDTH).astype(jnp.bfloat16)
```

```python
import functools
import math

import jax
import jax.numpy as jnp
from jax import lax
from jax.experimental import pallas as pl
from jax.experimental.pallas import tpu as pltpu
from jax.sharding import PartitionSpec as P

QUERY_SCALE = 144
LOG2_SCALE = QUERY_SCALE ** (-0.5) * math.log2(math.e)
HIDDEN = -1e30

HEADS = 8
CHUNKS = 4
PER = HEADS // CHUNKS
TALL = 144
PIECE = 2048

f32, bf16 = jnp.float32, jnp.bfloat16
MESH = pl.DeviceIdType.MESH
ROWS_BY_ROWS = (((1,), (1,)), ((), ()))


def place():
    kv, b = lax.axis_index("kv"), lax.axis_index("batch")
    return b % 4, (b // 4) * 2 + (kv // 2) % 2, kv // 4, kv % 2


def device(dx=0, dy=0, dz=0, e=0):
    x, y, z, c = place()
    x, y, z = (x + dx) % 4, (y + dy) % 4, (z + dz) % 8
    c = (c + e) % 2
    return (z * 2 + y % 2) * 2 + c, (y // 2) * 4 + x


def iota(shape, dim):
    return lax.broadcasted_iota(jnp.int32, shape, dim)


def one_hot(shape, wanted):
    return jnp.where(iota(shape, 1) == wanted(iota(shape, 0)), 1.0, 0.0).astype(bf16)


def dot(a, b):
    return jnp.dot(a, b, preferred_element_type=f32)


def dot_t(a, b):
    return lax.dot_general(a, b, ROWS_BY_ROWS, preferred_element_type=f32)


def in_two(v):
    high = v.astype(bf16).astype(f32)
    return high, (v - high).astype(bf16).astype(f32)


def packed_stats(mh, ml, total):
    lh, ll = in_two(total)
    row = iota((16, mh.shape[1]), 0)
    out = jnp.where(row == 0, mh, jnp.where(row == 1, ml, jnp.where(row == 2, lh, ll)))
    return jnp.where(row < 4, out, 0.0).astype(bf16)


def stats_of(block):
    st = block[128:TALL, :].astype(f32)
    return st[0:1] + st[1:2], st[2:3] + st[3:4]


def merged(blocks):
    stats = [stats_of(b) for b in blocks]
    top = functools.reduce(jnp.maximum, [m for m, _ in stats])
    out, total = 0.0, 0.0
    for b, (m, l) in zip(blocks, stats):
        w = jnp.exp2(m - top)
        out = out + b[0:128, :].astype(f32) * w
        total = total + l * w
    return out, top, total


def kernel(
    len_ref, q_hbm, k_hbm, v_hbm, sk_hbm, sv_hbm, out_ref,
    qin, kvin, sk, sv, kv, kvs, qy, qs, qsuf, xs, r1, x2, perm, ys, r2,
    so, sm, sl, suf, sufr, fin, finr, local_sem, send_sem, recv_sem,
):
    x, y, z, c = place()
    peers = [dict(dx=d, e=e) for d in (1, 3) for e in (0, 1)] + [dict(e=1)]
    peers += [dict(dy=d) for d in (1, 2, 3)] + [dict(dz=d, e=e) for d in range(1, 8) for e in (0, 1)]
    barrier = pltpu.get_barrier_semaphore()
    for p in peers:
        pl.semaphore_signal(barrier, inc=1, device_id=device(**p), device_id_type=MESH)

    loads = [
        pltpu.make_async_copy(src, dst, local_sem.at[i])
        for i, (src, dst) in enumerate(
            [(q_hbm, qin), (k_hbm, kvin.at[0]), (v_hbm, kvin.at[1]), (sk_hbm, sk), (sv_hbm, sv)]
        )
    ]
    for load in loads:
        load.start()

    started = []

    def send(src, dst, **to):
        i = len(started)
        copy = pltpu.make_async_remote_copy(
            src_ref=src, dst_ref=dst, send_sem=send_sem.at[i], recv_sem=recv_sem.at[i],
            device_id=device(**to), device_id_type=MESH,
        )
        copy.start()
        started.append(copy)
        return copy

    loads[0].wait()

    def query_row(row, e, g):
        j, r = (row % 8) // 2, row % 2
        return j * 32 + ((e + c) % 2 * 8 + g) * 2 + r

    q = qin[...]
    moved = dot(one_hot((128, 128), lambda o: query_row(o, o // 64, (o // 8) % 8)), q)
    qy[0, 0, 0] = moved[:64].astype(bf16).reshape(HEADS, 8, 128)
    qs[...] = moved[64:].astype(bf16).reshape(HEADS, 8, 128)
    qsuf[...] = dot(one_hot((128, 128), lambda o: query_row(o, (o // 8) % 2, o // 16)), q).astype(bf16)

    def head_row(o):
        big = o // 16
        return (o % 16) * 16 + (big // 8 + c) % 2 * 8 + big % 8

    move = one_hot((256, 256), head_row)
    loads[1].wait()
    loads[2].wait()
    for t in range(2):
        for b in range(4):
            m = dot(move, kvin[t, 256 * b : 256 * b + 256, :]).astype(bf16).reshape(16, 16, 128)
            kv[t, :, 0, 16 * b : 16 * b + 16, :] = m[:8]
            kvs[t, :, 16 * b : 16 * b + 16, :] = m[8:]

    pl.semaphore_wait(barrier, len(peers))

    def heads_of(k):
        return pl.ds(k * PER, PER)

    kv_copies = [dict() for _ in range(CHUNKS)]

    def send_kv(k):
        h = heads_of(k)
        for dx, e in ((1, 0), (3, 1), (1, 1), (3, 0), (0, 1)):
            src = kvs.at[:, h] if e else kv.at[:, h, 0]
            kv_copies[k][dx, e] = send(src, kv.at[:, h, 2 * dx + e], dx=dx, e=e)

    def forward_kv(k):
        h = heads_of(k)
        kv_copies[k][1, 0].wait_recv()
        kv_copies[k][2, 0] = send(kv.at[:, h, 2], kv.at[:, h, 4], dx=1)
        kv_copies[k][3, 1].wait_recv()
        kv_copies[k][2, 1] = send(kv.at[:, h, 7], kv.at[:, h, 5], dx=3)

    send_kv(0)
    q1 = []
    for dz in (4, 3, 5, 2, 6, 1, 7, 0):
        for e in (0, 1):
            if dz or e:
                q1.append(send(qs if e else qy.at[0, 0, 0], qy.at[0, dz, e], dz=dz, e=e))
    send_kv(1)

    so[...] = jnp.zeros_like(so)
    sl[...] = jnp.zeros_like(sl)
    sm[...] = jnp.full_like(sm, HIDDEN)
    loads[3].wait()
    loads[4].wait()
    length = len_ref[0]

    def suffix_piece(i, _):
        row, lane = iota((128, 128), 0), iota((128, 128), 1)
        head = ((row // 8) % 2 + c) % 2 * 8 + row // 16
        bias = jnp.where(lane % 16 == head, 0.0, HIDDEN)
        room = length - 3 + (row % 8) // 2 - lane // 16
        at = pl.ds(pl.multiple_of(i * PIECE, PIECE), PIECE)
        raw = dot_t(qsuf[...], sk[at, :])
        parts = []
        for t in range(PIECE // 128):
            part = raw[:, 128 * t : 128 * t + 128] * LOG2_SCALE + bias
            parts.append(jnp.where(room > i * (PIECE // 16) + 8 * t, part, HIDDEN))
        old = sm[...]
        top = jnp.maximum(old, jnp.max(functools.reduce(jnp.maximum, parts), 1, keepdims=True))
        weights = [jnp.exp2(part - top) for part in parts]
        shrink = jnp.exp2(old - top)
        sm[...] = top
        sl[...] = sl[...] * shrink + jnp.sum(functools.reduce(jnp.add, weights), 1, keepdims=True)
        rounded = jnp.concatenate([w.astype(bf16) for w in weights], axis=1)
        so[...] = so[...] * shrink + dot(rounded, sv[at, :])
        return 0

    lax.fori_loop(0, 3, suffix_piece, 0)
    forward_kv(0)
    send_kv(2)
    lax.fori_loop(3, 6, suffix_piece, 0)
    for copy in q1:
        copy.wait_recv()
    q2 = []

    def send_q(k):
        h = heads_of(k)
        q2.append([send(qy.at[0, :, :, h], qy.at[dy, :, :, h], dy=dy) for dy in (2, 1, 3)])

    for k in range(CHUNKS):
        send_q(k)
    forward_kv(1)
    send_kv(3)
    lax.fori_loop(6, 16384 // PIECE, suffix_piece, 0)

    eye = one_hot((128, 128), lambda o: o)
    mh, ml = in_two(sm[...])
    adjust = jnp.exp2(sm[...] - (mh + ml))
    lh, ll = in_two(sl[...] * adjust)
    suf[0:128, :] = dot_t(eye, (so[...] * adjust).astype(bf16)).astype(bf16)
    col = iota((128, 128), 1)
    columns = jnp.where(col == 0, mh, jnp.where(col == 1, ml, jnp.where(col == 2, lh, ll)))
    columns = jnp.where(col < 4, columns, 0.0).astype(bf16)
    suf[128:TALL, :] = dot_t(one_hot((16, 128), lambda o: o), columns).astype(bf16)
    suffix_copy = send(suf, sufr, e=1)
    for g in range(HEADS):
        perm[128 * g : 128 * g + 128, :] = one_hot(
            (128, 1024), lambda o, g=g: (o // 16) * 128 + g * 16 + o % 16
        )
    forward_kv(2)

    def prompt_head(g, _):
        keys = kv[0, g].reshape(512, 128)
        values = kv[1, g].reshape(512, 128)
        rows = qy[:, :, :, g].astype(f32).reshape(512, 128).astype(bf16)
        scores = dot_t(keys, rows) * LOG2_SCALE
        mh, ml = in_two(jnp.max(scores, 0, keepdims=True))
        weights = jnp.exp2(scores - (mh + ml))
        stats = packed_stats(mh, ml, jnp.sum(weights, 0, keepdims=True))
        out = dot(dot_t(eye, values).astype(bf16), weights.astype(bf16)).astype(bf16)
        for dy in range(4):
            xs[dy, g, 0:128, :] = out[:, 128 * dy : 128 * dy + 128]
            xs[dy, g, 128:TALL, :] = stats[:, 128 * dy : 128 * dy + 128]
        return 0

    rs1 = []
    for k in range(CHUNKS):
        for copy in q2[k]:
            copy.wait_recv()
        for at in ((0, 1), (1, 1), (3, 0), (2, 0), (2, 1)):
            kv_copies[k][at].wait_recv()
        lax.fori_loop(k * PER, (k + 1) * PER, prompt_head, 0)
        h = heads_of(k)
        rs1.append([send(xs.at[dy, h], r1.at[dy, h], dy=4 - dy) for dy in (2, 1, 3)])
        if k == 0:
            forward_kv(3)

    for k in range(CHUNKS):
        for copy in rs1[k]:
            copy.wait_recv()
        for g in range(k * PER, (k + 1) * PER):
            out, top, total = merged([xs[0, g]] + [r1[dy, g] for dy in range(1, 4)])
            mh, ml = in_two(top)
            adjust = jnp.exp2(top - (mh + ml))
            x2[0:128, 128 * g : 128 * g + 128] = (out * adjust).astype(bf16)
            x2[128:TALL, 128 * g : 128 * g + 128] = packed_stats(mh, ml, total * adjust)

    moved = dot(x2[...], perm[...]).astype(bf16)
    for dz in range(8):
        ys[dz] = moved[:, 128 * dz : 128 * dz + 128]
    rs2 = [send(ys.at[dz], r2.at[dz], dz=8 - dz) for dz in (4, 3, 5, 2, 6, 1, 7)]

    suffix_copy.wait_recv()
    lane = iota((TALL, 128), 1)
    own = jnp.where((lane // 8) % 2 == 0, suf[...].astype(f32), sufr[...].astype(f32))
    for copy in rs2:
        copy.wait_recv()
    out, _, total = merged([own, ys[0]] + [r2[dz] for dz in range(1, 8)])
    attended = (out / total).astype(bf16)

    def final_lane(o):
        e, j, g, r = o // 64, (o // 16) % 4, (o // 2) % 8, o % 2
        return g * 16 + e * 8 + j * 2 + r

    rows = dot_t(one_hot((128, 128), final_lane), attended).astype(bf16)
    fin[...] = rows[64:].reshape(4, 16, 128)
    last = send(fin, finr, e=1)
    out_ref[:, pl.ds(c, 1)] = rows[:64].reshape(4, 1, 16, 128)
    last.wait_recv()
    out_ref[:, pl.ds(1 - c, 1)] = finr[...].reshape(4, 1, 16, 128)
    for copy in started:
        copy.wait_send()


COPIES = 15 + 7 * CHUNKS + 3 * CHUNKS * 2 + 7 + 2


def body(queries, prefix_keys, prefix_values, suffix_keys, suffix_values, lengths):
    vmem, anyspace = pltpu.VMEM, pl.BlockSpec(memory_space=pl.ANY)
    out = pl.pallas_call(
        kernel,
        name="attend",
        out_shape=jax.ShapeDtypeStruct((4, 2, 16, 128), bf16),
        in_specs=[pl.BlockSpec(memory_space=pltpu.SMEM)] + [anyspace] * 5,
        out_specs=pl.BlockSpec(memory_space=vmem),
        scratch_shapes=[
            vmem((128, 128), bf16),
            vmem((2, 1024, 128), bf16),
            vmem((16384, 128), bf16),
            vmem((16384, 128), bf16),
            vmem((2, HEADS, 8, 64, 128), bf16),
            vmem((2, HEADS, 64, 128), bf16),
            vmem((4, 8, 2, HEADS, 8, 128), bf16),
            vmem((HEADS, 8, 128), bf16),
            vmem((128, 128), bf16),
            vmem((4, HEADS, TALL, 128), bf16),
            vmem((4, HEADS, TALL, 128), bf16),
            vmem((TALL, 1024), bf16),
            vmem((1024, 1024), bf16),
            vmem((8, TALL, 128), bf16),
            vmem((8, TALL, 128), bf16),
            vmem((128, 128), f32),
            vmem((128, 128), f32),
            vmem((128, 128), f32),
            vmem((TALL, 128), bf16),
            vmem((TALL, 128), bf16),
            vmem((4, 16, 128), bf16),
            vmem((4, 16, 128), bf16),
            pltpu.SemaphoreType.DMA((5,)),
            pltpu.SemaphoreType.DMA((COPIES,)),
            pltpu.SemaphoreType.DMA((COPIES,)),
        ],
        compiler_params=pltpu.CompilerParams(
            collective_id=0, has_side_effects=True, vmem_limit_bytes=48 * 2**20
        ),
    )(
        lengths,
        queries.reshape(128, 128),
        prefix_keys.reshape(1024, 128),
        prefix_values.reshape(1024, 128),
        suffix_keys.reshape(16384, 128),
        suffix_values.reshape(16384, 128),
    )
    return out.reshape(1, 4, 32, 128)


def solution(mesh):
    return jax.shard_map(
        body,
        mesh=mesh,
        in_specs=(
            P(("kv", "batch"), None, None, None),
            P(("kv", "batch"), None, None),
            P(("kv", "batch"), None, None),
            P(("kv", "batch"), None, None, None),
            P(("kv", "batch"), None, None, None),
            P(("kv", "batch")),
        ),
        out_specs=P(("kv", "batch"), None, None, None),
        check_vma=False,
    )
```

```python
import functools
import math

import jax
import jax.numpy as jnp
from jax import lax
from jax.experimental import pallas as pl
from jax.experimental.pallas import tpu as pltpu
from jax.sharding import PartitionSpec as P

QUERY_SCALE = 144
LOG2_SCALE = QUERY_SCALE ** (-0.5) * math.log2(math.e)
HIDDEN = -1e30

HEADS = 8
CHUNKS = 4
PER = HEADS // CHUNKS
TALL = 144
PIECE = 2048

f32, bf16 = jnp.float32, jnp.bfloat16
MESH = pl.DeviceIdType.MESH
ROWS_BY_ROWS = (((1,), (1,)), ((), ()))


def place():
    kv, b = lax.axis_index("kv"), lax.axis_index("batch")
    return b % 4, (b // 4) * 2 + (kv // 2) % 2, kv // 4, kv % 2


def device(dx=0, dy=0, dz=0, e=0):
    x, y, z, c = place()
    x, y, z = (x + dx) % 4, (y + dy) % 4, (z + dz) % 8
    c = (c + e) % 2
    return (z * 2 + y % 2) * 2 + c, (y // 2) * 4 + x


def iota(shape, dim):
    return lax.broadcasted_iota(jnp.int32, shape, dim)


def one_hot(shape, wanted):
    return jnp.where(iota(shape, 1) == wanted(iota(shape, 0)), 1.0, 0.0).astype(bf16)


def dot(a, b):
    return jnp.dot(a, b, preferred_element_type=f32)


def dot_t(a, b):
    return lax.dot_general(a, b, ROWS_BY_ROWS, preferred_element_type=f32)


def in_two(v):
    high = v.astype(bf16).astype(f32)
    return high, (v - high).astype(bf16).astype(f32)


def packed_stats(mh, ml, total):
    lh, ll = in_two(total)
    row = iota((16, mh.shape[1]), 0)
    out = jnp.where(row == 0, mh, jnp.where(row == 1, ml, jnp.where(row == 2, lh, ll)))
    return jnp.where(row < 4, out, 0.0).astype(bf16)


def stats_of(block):
    st = block[128:TALL, :].astype(f32)
    return st[0:1] + st[1:2], st[2:3] + st[3:4]


def merged(blocks):
    stats = [stats_of(b) for b in blocks]
    top = functools.reduce(jnp.maximum, [m for m, _ in stats])
    out, total = 0.0, 0.0
    for b, (m, l) in zip(blocks, stats):
        w = jnp.exp2(m - top)
        out = out + b[0:128, :].astype(f32) * w
        total = total + l * w
    return out, top, total


def kernel(
    len_ref, q_hbm, k_hbm, v_hbm, sk_hbm, sv_hbm, out_ref,
    qin, kvin, sk, sv, kv, kvs, qy, qs, qsuf, xs, r1, sx, ys, r2,
    so, sm, sl, local_sem, send_sem, recv_sem,
):
    x, y, z, c = place()
    peers = [dict(dx=d, e=e) for d in (1, 3) for e in (0, 1)] + [dict(e=1)]
    peers += [dict(dy=d, e=e) for d in (1, 2, 3) for e in (0, 1)]
    peers += [dict(dz=d, e=e) for d in range(1, 8) for e in (0, 1)]
    barrier = pltpu.get_barrier_semaphore()
    for p in peers:
        pl.semaphore_signal(barrier, inc=1, device_id=device(**p), device_id_type=MESH)

    loads = [
        pltpu.make_async_copy(src, dst, local_sem.at[i])
        for i, (src, dst) in enumerate(
            [(k_hbm, kvin.at[0]), (v_hbm, kvin.at[1]), (q_hbm, qin), (sk_hbm, sk), (sv_hbm, sv)]
        )
    ]
    for load in loads:
        load.start()

    started = []

    def send(src, dst, **to):
        i = len(started)
        copy = pltpu.make_async_remote_copy(
            src_ref=src, dst_ref=dst, send_sem=send_sem.at[i], recv_sem=recv_sem.at[i],
            device_id=device(**to), device_id_type=MESH,
        )
        copy.start()
        started.append(copy)
        return copy

    def heads_of(k, n=1):
        return pl.ds(k * PER, n * PER)

    def head_row(o):
        big = o // 16
        return (o % 16) * 16 + (big // 8 + c) % 2 * 8 + big % 8

    move = one_hot((256, 256), head_row)
    for t in range(2):
        loads[t].wait()
        for b in range(4):
            m = dot(move, kvin[t, 256 * b : 256 * b + 256, :]).astype(bf16).reshape(16, 16, 128)
            kv[t, :, 0, 16 * b : 16 * b + 16, :] = m[:8]
            kvs[t, :, 16 * b : 16 * b + 16, :] = m[8:]

    loads[2].wait()

    def query_row(o):
        e, g, j, r = o // 64, (o // 8) % 8, (o % 8) // 2, o % 2
        return j * 32 + ((e + c) % 2 * 8 + g) * 2 + r

    q = dot(one_hot((128, 128), query_row), qin[...]).astype(bf16)
    qsuf[...] = q
    qy[0, 0, 0] = q[:64].reshape(HEADS, 8, 128)
    qs[...] = q[64:].reshape(HEADS, 8, 128)

    pl.semaphore_wait(barrier, len(peers))

    kv_copies = [dict() for _ in range(CHUNKS)]

    def send_kv(k):
        h = heads_of(k)
        for dx, e in ((1, 0), (3, 1), (1, 1), (3, 0), (0, 1)):
            src = kvs.at[:, h] if e else kv.at[:, h, 0]
            kv_copies[k][dx, e] = send(src, kv.at[:, h, 2 * dx + e], dx=dx, e=e)

    def forward_kv(k):
        h = heads_of(k)
        kv_copies[k][1, 0].wait_recv()
        kv_copies[k][2, 0] = send(kv.at[:, h, 2], kv.at[:, h, 4], dx=1)
        kv_copies[k][3, 1].wait_recv()
        kv_copies[k][2, 1] = send(kv.at[:, h, 7], kv.at[:, h, 5], dx=3)

    half = CHUNKS // 2
    zy, yz = heads_of(0, half), heads_of(half, half)

    def source(e, h):
        return qs.at[h] if e else qy.at[0, 0, 0, h]

    send_kv(0)
    q1 = [
        send(source(e, zy), qy.at[0, dz, e, zy], dz=dz, e=e)
        for dz in (4, 3, 5, 2, 6, 1, 7, 0) for e in (0, 1) if dz or e
    ]
    p1 = [
        send(source(e, yz), qy.at[dy, 0, e, yz], dy=dy, e=e)
        for dy in (2, 1, 3, 0) for e in (0, 1) if dy or e
    ]
    send_kv(1)

    so[...] = jnp.zeros_like(so)
    sl[...] = jnp.zeros_like(sl)
    sm[...] = jnp.full_like(sm, HIDDEN)
    sx[...] = jnp.zeros_like(sx)
    loads[3].wait()
    loads[4].wait()
    length = len_ref[0]

    def suffix_piece(i, _):
        row, lane = iota((128, 128), 0), iota((128, 128), 1)
        head = (row // 64 + c) % 2 * 8 + (row // 8) % 8
        bias = jnp.where(lane % 16 == head, 0.0, HIDDEN)
        room = length - 3 + (row % 8) // 2 - lane // 16
        at = pl.ds(pl.multiple_of(i * PIECE, PIECE), PIECE)
        raw = dot_t(qsuf[...], sk[at, :])
        parts = []
        for t in range(PIECE // 128):
            part = raw[:, 128 * t : 128 * t + 128] * LOG2_SCALE + bias
            parts.append(jnp.where(room > i * (PIECE // 16) + 8 * t, part, HIDDEN))
        old = sm[...]
        top = jnp.maximum(old, jnp.max(functools.reduce(jnp.maximum, parts), 1, keepdims=True))
        weights = [jnp.exp2(part - top) for part in parts]
        shrink = jnp.exp2(old - top)
        sm[...] = top
        sl[...] = sl[...] * shrink + jnp.sum(functools.reduce(jnp.add, weights), 1, keepdims=True)
        rounded = jnp.concatenate([w.astype(bf16) for w in weights], axis=1)
        so[...] = so[...] * shrink + dot(rounded, sv[at, :])
        return 0

    def suffix(first, last):
        lax.fori_loop(first, last, suffix_piece, 0)

    suffix(0, 2)
    for copy in p1:
        copy.wait_recv()
    q2 = [[] for _ in range(CHUNKS)]

    def send_q_z(k):
        h = heads_of(k)
        q2[k] = [send(qy.at[:, 0, :, h], qy.at[:, dz, :, h], dz=dz) for dz in (4, 3, 5, 2, 6, 1, 7)]

    def send_q_y(k):
        h = heads_of(k)
        q2[k] = [send(qy.at[0, :, :, h], qy.at[dy, :, :, h], dy=dy) for dy in (2, 1, 3)]

    for k in range(half, CHUNKS):
        send_q_z(k)
    suffix(2, 3)
    forward_kv(0)
    send_kv(2)
    suffix(3, 5)
    for copy in q1:
        copy.wait_recv()
    for k in range(half):
        send_q_y(k)
    suffix(5, 6)
    forward_kv(1)
    send_kv(3)
    suffix(6, 16384 // PIECE)
    forward_kv(2)

    eye = one_hot((128, 128), lambda o: o)

    def prompt_head(g, _):
        keys = kv[0, g].reshape(512, 128)
        values = kv[1, g].reshape(512, 128)
        rows = qy[:, :, :, g].astype(f32).reshape(512, 128).astype(bf16)
        scores = dot_t(keys, rows) * LOG2_SCALE
        mh, ml = in_two(jnp.max(scores, 0, keepdims=True))
        weights = jnp.exp2(scores - (mh + ml))
        stats = packed_stats(mh, ml, jnp.sum(weights, 0, keepdims=True))
        out = dot(dot_t(eye, values).astype(bf16), weights.astype(bf16)).astype(bf16)
        for dy in range(4):
            xs[dy, g, 0:128, :] = out[:, 128 * dy : 128 * dy + 128]
            xs[dy, g, 128:TALL, :] = stats[:, 128 * dy : 128 * dy + 128]
        return 0

    rs1 = []
    rs2 = []

    def over_y(k):
        for copy in rs1[k]:
            copy.wait_recv()
        for i in range(PER):
            g = k * PER + i
            out, top, total = merged([xs[0, g]] + [r1[dy, g] for dy in range(1, 4)])
            mh, ml = in_two(top)
            adjust = jnp.exp2(top - (mh + ml))
            ys[k, :, i] = dot_t(eye, (out * adjust).astype(bf16)).astype(bf16).reshape(16, 8, 128)
            sx[k, 16 * i : 16 * i + 16, :] = packed_stats(mh, ml, total * adjust)
        ys[k, :, PER] = dot_t(eye, sx[k]).astype(bf16).reshape(16, 8, 128)
        rs2.append(
            [
                send(ys.at[k, 2 * dz + e], r2.at[k, 2 * dz + e], dz=8 - dz, e=e)
                for dz in (4, 3, 5, 2, 6, 1, 7, 0) for e in (0, 1) if dz or e
            ]
        )

    for k in range(CHUNKS):
        for copy in q2[k]:
            copy.wait_recv()
        for at in ((0, 1), (1, 1), (3, 0), (2, 0), (2, 1)):
            kv_copies[k][at].wait_recv()
        lax.fori_loop(k * PER, (k + 1) * PER, prompt_head, 0)
        h = heads_of(k)
        rs1.append([send(xs.at[dy, h], r1.at[dy, h], dy=4 - dy) for dy in (2, 1, 3)])
        if k == 0:
            forward_kv(3)
        if k >= 2:
            over_y(k - 2)
    for k in range(CHUNKS - 2, CHUNKS):
        over_y(k)

    done = []
    for k in range(CHUNKS):
        for copy in rs2[k]:
            copy.wait_recv()
        for e in (0, 1):
            blocks = [ys.at[k, 0] if not (dz or e) else r2.at[k, 2 * dz + e] for dz in range(8)]
            lane = iota((8, 128), 1)
            mine = [(e * 8 + k * PER + i) * 8 for i in range(PER)]
            top_own = total_own = jnp.zeros((8, 128), f32)
            for i, at in enumerate(mine):
                top_own = jnp.where(lane // 16 == i, sm[at : at + 8, :], top_own)
                total_own = jnp.where(lane // 16 == i, sl[at : at + 8, :], total_own)
            tiles = [b[PER].astype(f32) for b in blocks]
            tops = [t + pltpu.roll(t, 127, 1) for t in tiles] + [top_own]
            totals = [pltpu.roll(t, 126, 1) + pltpu.roll(t, 125, 1) for t in tiles] + [total_own]
            top = functools.reduce(jnp.maximum, tops)
            factors = [jnp.exp2(t - top) for t in tops]
            whole = functools.reduce(jnp.add, [f * t for f, t in zip(factors, totals)])
            factors = [f / whole for f in factors]
            for i, at in enumerate(mine):
                parts = [b[i].astype(f32) for b in blocks] + [so[at : at + 8, :]]
                out = functools.reduce(
                    jnp.add, [p * f[:, 16 * i : 16 * i + 1] for p, f in zip(parts, factors)]
                )
                so[at : at + 8, :] = out

    def final_row(o):
        j, g, r = o // 32, (o // 2) % 16, o % 2
        return (g // 8 + c) % 2 * 64 + g % 8 * 8 + j * 2 + r

    out_ref[...] = dot(one_hot((128, 128), final_row), so[...].astype(bf16)).astype(bf16)
    for copy in started:
        copy.wait_send()


COPIES = 15 + 7 + 7 * CHUNKS + 3 * (CHUNKS // 2) + 7 * (CHUNKS - CHUNKS // 2) + 3 * CHUNKS + 15 * CHUNKS


def body(queries, prefix_keys, prefix_values, suffix_keys, suffix_values, lengths):
    vmem, anyspace = pltpu.VMEM, pl.BlockSpec(memory_space=pl.ANY)
    out = pl.pallas_call(
        kernel,
        name="attend",
        out_shape=jax.ShapeDtypeStruct((128, 128), bf16),
        in_specs=[pl.BlockSpec(memory_space=pltpu.SMEM)] + [anyspace] * 5,
        out_specs=pl.BlockSpec(memory_space=vmem),
        scratch_shapes=[
            vmem((128, 128), bf16),
            vmem((2, 1024, 128), bf16),
            vmem((16384, 128), bf16),
            vmem((16384, 128), bf16),
            vmem((2, HEADS, 8, 64, 128), bf16),
            vmem((2, HEADS, 64, 128), bf16),
            vmem((4, 8, 2, HEADS, 8, 128), bf16),
            vmem((HEADS, 8, 128), bf16),
            vmem((128, 128), bf16),
            vmem((4, HEADS, TALL, 128), bf16),
            vmem((4, HEADS, TALL, 128), bf16),
            vmem((CHUNKS, 128, 128), bf16),
            vmem((CHUNKS, 16, PER + 1, 8, 128), bf16),
            vmem((CHUNKS, 16, PER + 1, 8, 128), bf16),
            vmem((128, 128), f32),
            vmem((128, 128), f32),
            vmem((128, 128), f32),
            pltpu.SemaphoreType.DMA((5,)),
            pltpu.SemaphoreType.DMA((COPIES,)),
            pltpu.SemaphoreType.DMA((COPIES,)),
        ],
        compiler_params=pltpu.CompilerParams(
            collective_id=0, has_side_effects=True, vmem_limit_bytes=67_043_328
        ),
    )(
        lengths,
        queries.reshape(128, 128),
        prefix_keys.reshape(1024, 128),
        prefix_values.reshape(1024, 128),
        suffix_keys.reshape(16384, 128),
        suffix_values.reshape(16384, 128),
    )
    return out.reshape(1, 4, 32, 128)


def solution(mesh):
    return jax.shard_map(
        body,
        mesh=mesh,
        in_specs=(
            P(("kv", "batch"), None, None, None),
            P(("kv", "batch"), None, None),
            P(("kv", "batch"), None, None),
            P(("kv", "batch"), None, None, None),
            P(("kv", "batch"), None, None, None),
            P(("kv", "batch")),
        ),
        out_specs=P(("kv", "batch"), None, None, None),
        check_vma=False,
    )
```

```python
import functools
import math

import jax
import jax.numpy as jnp
from jax import lax
from jax.experimental import pallas as pl
from jax.experimental.pallas import tpu as pltpu
from jax.sharding import PartitionSpec as P

QUERY_SCALE = 144
LOG2_SCALE = QUERY_SCALE ** (-0.5) * math.log2(math.e)
HIDDEN = -1e30

HEADS = 8
SIZES = (1, 1, 2, 2, 1, 1)
STARTS = tuple(sum(SIZES[:k]) for k in range(len(SIZES)))
CHUNKS = len(SIZES)
EARLY = 3
LAST = (3, 3, 3, 3, 5, 5)
TAILS = tuple(sorted(set(LAST)))


def tile_of(head):
    return head + sum(STARTS[t] + SIZES[t] <= head for t in TAILS)


TILES = HEADS + len(TAILS)
SEMS = 3 + 4 * CHUNKS
TALL = 144
PIECE = 2048

f32, bf16 = jnp.float32, jnp.bfloat16
MESH = pl.DeviceIdType.MESH
ROWS_BY_ROWS = (((1,), (1,)), ((), ()))


def place():
    kv, b = lax.axis_index("kv"), lax.axis_index("batch")
    return b % 4, (b // 4) * 2 + (kv // 2) % 2, kv // 4, kv % 2


def device(dx=0, dy=0, dz=0, e=0):
    x, y, z, c = place()
    x, y, z = (x + dx) % 4, (y + dy) % 4, (z + dz) % 8
    c = (c + e) % 2
    return (z * 2 + y % 2) * 2 + c, (y // 2) * 4 + x


def iota(shape, dim):
    return lax.broadcasted_iota(jnp.int32, shape, dim)


def one_hot(shape, wanted):
    return jnp.where(iota(shape, 1) == wanted(iota(shape, 0)), 1.0, 0.0).astype(bf16)


def dot(a, b):
    return jnp.dot(a, b, preferred_element_type=f32)


def dot_t(a, b):
    return lax.dot_general(a, b, ROWS_BY_ROWS, preferred_element_type=f32)


def in_two(v):
    high = v.astype(bf16).astype(f32)
    return high, (v - high).astype(bf16).astype(f32)


def packed_stats(mh, ml, total):
    lh, ll = in_two(total)
    row = iota((16, mh.shape[1]), 0)
    out = jnp.where(row == 0, mh, jnp.where(row == 1, ml, jnp.where(row == 2, lh, ll)))
    return jnp.where(row < 4, out, 0.0).astype(bf16)


def stats_of(block):
    st = block[128:TALL, :].astype(f32)
    return st[0:1] + st[1:2], st[2:3] + st[3:4]


def merged(blocks):
    stats = [stats_of(b) for b in blocks]
    top = functools.reduce(jnp.maximum, [m for m, _ in stats])
    out, total = 0.0, 0.0
    for b, (m, l) in zip(blocks, stats):
        w = jnp.exp2(m - top)
        out = out + b[0:128, :].astype(f32) * w
        total = total + l * w
    return out, top, total


def kernel(
    len_ref, q_hbm, k_hbm, v_hbm, sk_hbm, sv_hbm, out_ref,
    qin, kvin, sk, sv, kv, kvs, qy, qs, qsuf, xs, r1, sx, ys, r2,
    so, sm, sl, local_sem, send_sem, recv_sem,
):
    x, y, z, c = place()
    loads = [
        pltpu.make_async_copy(src, dst, local_sem.at[i])
        for i, (src, dst) in enumerate(
            [(k_hbm, kvin.at[0]), (v_hbm, kvin.at[1]), (q_hbm, qin), (sk_hbm, sk), (sv_hbm, sv)]
        )
    ]
    for load in loads:
        load.start()

    peers = [dict(dx=d, e=e) for d in (1, 3) for e in (0, 1)] + [dict(e=1)]
    peers += [dict(dy=d, e=e) for d in (1, 2, 3) for e in (0, 1)]
    peers += [dict(dz=d, e=e) for d in range(1, 8) for e in (0, 1)]
    barrier = pltpu.get_barrier_semaphore()
    for p in peers:
        pl.semaphore_signal(barrier, inc=1, device_id=device(**p), device_id_type=MESH)

    groups = []

    def send(group, src, dst, sem=None, **to):
        pltpu.make_async_remote_copy(
            src_ref=src, dst_ref=dst, send_sem=send_sem.at[group],
            recv_sem=recv_sem.at[group if sem is None else sem],
            device_id=device(**to), device_id_type=MESH,
        ).start()

    def new_group(arrivals):
        groups.append(arrivals)
        return len(groups) - 1

    def wait_for(sem, ref):
        pltpu.make_async_copy(ref, ref, sem).wait()

    def arrived(group):
        wait_for(recv_sem.at[group], groups[group])

    def heads_of(k, last=None):
        return pl.ds(STARTS[k], sum(SIZES[k : (k if last is None else last) + 1]))

    def head_row(o):
        big = o // 16
        return (o % 16) * 16 + (big // 8 + c) % 2 * 8 + big % 8

    move = one_hot((256, 256), head_row)
    for t in range(2):
        loads[t].wait()
        for b in range(4):
            m = dot(move, kvin[t, 256 * b : 256 * b + 256, :]).astype(bf16).reshape(16, 16, 128)
            kv[t, :, 0, 16 * b : 16 * b + 16, :] = m[:8]
            kvs[t, :, 16 * b : 16 * b + 16, :] = m[8:]

    loads[2].wait()

    def query_row(o):
        e, g, j, r = o // 64, (o // 8) % 8, (o % 8) // 2, o % 2
        return j * 32 + ((e + c) % 2 * 8 + g) * 2 + r

    q = dot(one_hot((128, 128), query_row), qin[...]).astype(bf16)
    qsuf[...] = q
    qy[0, 0, 0] = q[:64].reshape(HEADS, 8, 128)
    qs[...] = q[64:].reshape(HEADS, 8, 128)

    pl.semaphore_wait(barrier, len(peers))

    kv_groups = [new_group(kv.at[:, heads_of(k), 1:8]) for k in range(CHUNKS)]

    def send_kv(k):
        h = heads_of(k)
        for dx, e in ((1, 0), (3, 1), (1, 1), (3, 0), (0, 1)):
            src = kvs.at[:, h] if e else kv.at[:, h, 0]
            relayed = {(1, 0): SEMS + k, (3, 1): SEMS + CHUNKS + k}.get((dx, e))
            send(kv_groups[k], src, kv.at[:, h, 2 * dx + e], sem=relayed, dx=dx, e=e)

    def forward_kv(k):
        h = heads_of(k)
        wait_for(recv_sem.at[SEMS + k], kv.at[:, h, 2])
        send(kv_groups[k], kv.at[:, h, 2], kv.at[:, h, 4], dx=1)
        wait_for(recv_sem.at[SEMS + CHUNKS + k], kv.at[:, h, 7])
        send(kv_groups[k], kv.at[:, h, 7], kv.at[:, h, 5], dx=3)

    def kv_arrived(k):
        wait_for(recv_sem.at[kv_groups[k]], kv.at[:, heads_of(k), 1:6])

    zy, yz = heads_of(1, EARLY - 1), heads_of(EARLY, CHUNKS - 1)

    def source(e, h):
        return qs.at[h] if e else qy.at[0, 0, 0, h]

    def send_q1(h, n):
        group = new_group(r2.at[1:16, 0:n])
        for dz in (4, 3, 5, 2, 6, 1, 7, 0):
            for e in (0, 1):
                if dz or e:
                    send(group, source(e, h), qy.at[0, dz, e, h], dz=dz, e=e)
        return group

    send_kv(0)
    q1a = send_q1(heads_of(0), SIZES[0])
    p1 = new_group(r2.at[1:8, 0 : HEADS - STARTS[EARLY]])
    for dy in (2, 1, 3, 0):
        for e in (0, 1):
            if dy or e:
                send(p1, source(e, yz), qy.at[dy, 0, e, yz], dy=dy, e=e)
    q1b = send_q1(zy, STARTS[EARLY] - STARTS[1])
    send_kv(1)

    so[...] = jnp.zeros_like(so)
    sl[...] = jnp.zeros_like(sl)
    sm[...] = jnp.full_like(sm, HIDDEN)
    sx[...] = jnp.zeros_like(sx)
    loads[3].wait()
    loads[4].wait()
    length = len_ref[0]

    def suffix_piece(i, _):
        row, lane = iota((128, 128), 0), iota((128, 128), 1)
        head = (row // 64 + c) % 2 * 8 + (row // 8) % 8
        bias = jnp.where(lane % 16 == head, 0.0, HIDDEN)
        room = length - 3 + (row % 8) // 2 - lane // 16
        at = pl.ds(pl.multiple_of(i * PIECE, PIECE), PIECE)
        raw = dot_t(qsuf[...], sk[at, :])
        parts = []
        for t in range(PIECE // 128):
            part = raw[:, 128 * t : 128 * t + 128] * LOG2_SCALE + bias
            parts.append(jnp.where(room > i * (PIECE // 16) + 8 * t, part, HIDDEN))
        old = sm[...]
        top = jnp.maximum(old, jnp.max(functools.reduce(jnp.maximum, parts), 1, keepdims=True))
        weights = [jnp.exp2(part - top) for part in parts]
        shrink = jnp.exp2(old - top)
        sm[...] = top
        sl[...] = sl[...] * shrink + jnp.sum(functools.reduce(jnp.add, weights), 1, keepdims=True)
        rounded = jnp.concatenate([w.astype(bf16) for w in weights], axis=1)
        so[...] = so[...] * shrink + dot(rounded, sv[at, :])
        return 0

    def suffix(first, last):
        lax.fori_loop(first, last, suffix_piece, 0)

    q2 = {}

    def send_q_z(k):
        h = heads_of(k)
        q2[k] = new_group(qy.at[:, 1:8, :, h])
        for dz in (4, 3, 5, 2, 6, 1, 7):
            send(q2[k], qy.at[:, 0, :, h], qy.at[:, dz, :, h], dz=dz)

    def send_q_y(k):
        h = heads_of(k)
        q2[k] = new_group(qy.at[1:4, :, :, h])
        for dy in (2, 1, 3):
            send(q2[k], qy.at[0, :, :, h], qy.at[dy, :, :, h], dy=dy)

    suffix(0, 2)
    forward_kv(0)
    send_kv(2)
    arrived(p1)
    for k in range(EARLY, CHUNKS):
        send_q_z(k)
    suffix(2, 3)
    arrived(q1a)
    send_q_y(0)
    forward_kv(1)
    send_kv(3)
    suffix(3, 4)
    arrived(q1b)
    for k in range(1, EARLY):
        send_q_y(k)
    suffix(4, 6)
    forward_kv(2)
    send_kv(4)
    send_kv(5)
    suffix(6, 16384 // PIECE)

    eye = one_hot((128, 128), lambda o: o)

    def prompt_head(g, _):
        keys = kv[0, g].reshape(512, 128)
        values = kv[1, g].reshape(512, 128)
        rows = qy[:, :, :, g].astype(f32).reshape(512, 128).astype(bf16)
        scores = dot_t(keys, rows) * LOG2_SCALE
        mh, ml = in_two(jnp.max(scores, 0, keepdims=True))
        weights = jnp.exp2(scores - (mh + ml))
        stats = packed_stats(mh, ml, jnp.sum(weights, 0, keepdims=True))
        out = dot(dot_t(eye, values).astype(bf16), weights.astype(bf16)).astype(bf16)
        for dy in range(4):
            xs[dy, g, 0:128, :] = out[:, 128 * dy : 128 * dy + 128]
            xs[dy, g, 128:TALL, :] = stats[:, 128 * dy : 128 * dy + 128]
        return 0

    rs1 = []
    rs2 = []

    def over_y(k):
        arrived(rs1[k])
        first, n = tile_of(STARTS[k]), SIZES[k]
        for i in range(n):
            g = STARTS[k] + i
            out, top, total = merged([xs[0, g]] + [r1[dy, g] for dy in range(1, 4)])
            mh, ml = in_two(top)
            adjust = jnp.exp2(top - (mh + ml))
            ys[:, first + i] = dot_t(eye, (out * adjust).astype(bf16)).astype(bf16).reshape(16, 8, 128)
            sx[TAILS.index(LAST[k]), 16 * g : 16 * g + 16, :] = packed_stats(mh, ml, total * adjust)
        if k in TAILS:
            stats = dot_t(eye, sx[TAILS.index(k)]).astype(bf16)
            ys[:, first + n] = stats.reshape(16, 8, 128)
            n += 1
        t = pl.ds(first, n)
        rs2.append(new_group(r2.at[1:16, t]))
        for dz in (4, 3, 5, 2, 6, 1, 7, 0):
            for e in (0, 1):
                if dz or e:
                    send(rs2[k], ys.at[2 * dz + e, t], r2.at[2 * dz + e, t], dz=8 - dz, e=e)

    def prompt(k):
        arrived(q2[k])
        kv_arrived(k)
        lax.fori_loop(STARTS[k], STARTS[k] + SIZES[k], prompt_head, 0)
        h = heads_of(k)
        rs1.append(new_group(r1.at[1:4, h]))
        for dy in (2, 1, 3):
            send(rs1[k], xs.at[dy, h], r1.at[dy, h], dy=4 - dy)

    prompt(0)
    prompt(1)
    forward_kv(3)
    forward_kv(4)
    prompt(2)
    forward_kv(5)
    over_y(0)
    over_y(1)
    prompt(3)
    prompt(4)
    prompt(5)
    for k in range(2, CHUNKS):
        over_y(k)

    begun = 0
    for tail in TAILS:
        mine = range(begun, tail + 1)
        begun = tail + 1
        for k in mine:
            arrived(rs2[k])
        heads = range(STARTS[mine[0]], STARTS[tail] + SIZES[tail])
        at_stats = tile_of(heads[-1]) + 1
        for e in (0, 1):
            blocks = [r2.at[2 * dz + e] if dz or e else ys.at[0] for dz in range(8)]
            lane = iota((8, 128), 1)
            top_own = total_own = jnp.zeros((8, 128), f32)
            for g in heads:
                at = (e * 8 + g) * 8
                top_own = jnp.where(lane // 16 == g, sm[at : at + 8, :], top_own)
                total_own = jnp.where(lane // 16 == g, sl[at : at + 8, :], total_own)
            tiles = [b[at_stats].astype(f32) for b in blocks]
            tops = [t + pltpu.roll(t, 127, 1) for t in tiles] + [top_own]
            totals = [pltpu.roll(t, 126, 1) + pltpu.roll(t, 125, 1) for t in tiles] + [total_own]
            top = functools.reduce(jnp.maximum, tops)
            factors = [jnp.exp2(t - top) for t in tops]
            whole = functools.reduce(jnp.add, [f * t for f, t in zip(factors, totals)])
            factors = [f / whole for f in factors]
            for g in heads:
                at = (e * 8 + g) * 8
                parts = [b[tile_of(g)].astype(f32) for b in blocks] + [so[at : at + 8, :]]
                so[at : at + 8, :] = functools.reduce(
                    jnp.add, [p * f[:, 16 * g : 16 * g + 1] for p, f in zip(parts, factors)]
                )

    def final_row(o):
        j, g, r = o // 32, (o // 2) % 16, o % 2
        return (g // 8 + c) % 2 * 64 + g % 8 * 8 + j * 2 + r

    out_ref[...] = dot(one_hot((128, 128), final_row), so[...].astype(bf16)).astype(bf16)
    for group, arrivals in enumerate(groups):
        wait_for(send_sem.at[group], arrivals)


def body(queries, prefix_keys, prefix_values, suffix_keys, suffix_values, lengths):
    vmem, anyspace = pltpu.VMEM, pl.BlockSpec(memory_space=pltpu.HBM)
    out = pl.pallas_call(
        kernel,
        name="attend",
        out_shape=jax.ShapeDtypeStruct((128, 128), bf16),
        in_specs=[pl.BlockSpec(memory_space=pltpu.SMEM)] + [anyspace] * 5,
        out_specs=pl.BlockSpec(memory_space=vmem),
        scratch_shapes=[
            vmem((128, 128), bf16),
            vmem((2, 1024, 128), bf16),
            vmem((16384, 128), bf16),
            vmem((16384, 128), bf16),
            vmem((2, HEADS, 8, 64, 128), bf16),
            vmem((2, HEADS, 64, 128), bf16),
            vmem((4, 8, 2, HEADS, 8, 128), bf16),
            vmem((HEADS, 8, 128), bf16),
            vmem((128, 128), bf16),
            vmem((4, HEADS, TALL, 128), bf16),
            vmem((4, HEADS, TALL, 128), bf16),
            vmem((len(TAILS), 128, 128), bf16),
            vmem((16, TILES, 8, 128), bf16),
            vmem((16, TILES, 8, 128), bf16),
            vmem((128, 128), f32),
            vmem((128, 128), f32),
            vmem((128, 128), f32),
            pltpu.SemaphoreType.DMA((5,)),
            pltpu.SemaphoreType.DMA((SEMS,)),
            pltpu.SemaphoreType.DMA((SEMS + 2 * CHUNKS,)),
        ],
        compiler_params=pltpu.CompilerParams(
            collective_id=0, has_side_effects=True, vmem_limit_bytes=67_043_328
        ),
    )(
        lengths,
        queries.reshape(128, 128),
        prefix_keys.reshape(1024, 128),
        prefix_values.reshape(1024, 128),
        suffix_keys.reshape(16384, 128),
        suffix_values.reshape(16384, 128),
    )
    return out.reshape(1, 4, 32, 128)


def solution(mesh):
    return jax.shard_map(
        body,
        mesh=mesh,
        in_specs=(
            P(("kv", "batch"), None, None, None),
            P(("kv", "batch"), None, None),
            P(("kv", "batch"), None, None),
            P(("kv", "batch"), None, None, None),
            P(("kv", "batch"), None, None, None),
            P(("kv", "batch")),
        ),
        out_specs=P(("kv", "batch"), None, None, None),
        check_vma=False,
    )
```

```python
import functools
import math

import jax
import jax.numpy as jnp
from jax import lax
from jax.experimental import pallas as pl
from jax.experimental.pallas import tpu as pltpu
from jax.sharding import PartitionSpec as P

QUERY_SCALE = 144
LOG2_SCALE = QUERY_SCALE ** (-0.5) * math.log2(math.e)
HIDDEN = -1e30

HEADS = 8
SIZES = (1,) * HEADS
STARTS = tuple(sum(SIZES[:k]) for k in range(len(SIZES)))
CHUNKS = len(SIZES)
EARLY = 4
LAST = (3,) * 4 + (7,) * 4
TAILS = tuple(sorted(set(LAST)))


def tile_of(head):
    return head + sum(STARTS[t] + SIZES[t] <= head for t in TAILS)


TILES = HEADS + len(TAILS)
SEMS = 3 + 4 * CHUNKS
TALL = 136
PIECE = 2048

f32, bf16 = jnp.float32, jnp.bfloat16
MESH = pl.DeviceIdType.MESH
ROWS_BY_ROWS = (((1,), (1,)), ((), ()))


def place():
    kv, b = lax.axis_index("kv"), lax.axis_index("batch")
    return b % 4, (b // 4) * 2 + (kv // 2) % 2, kv // 4, kv % 2


def device(dx=0, dy=0, dz=0, e=0):
    x, y, z, c = place()
    x, y, z = (x + dx) % 4, (y + dy) % 4, (z + dz) % 8
    c = (c + e) % 2
    return (z * 2 + y % 2) * 2 + c, (y // 2) * 4 + x


def iota(shape, dim):
    return lax.broadcasted_iota(jnp.int32, shape, dim)


def one_hot(shape, wanted):
    return jnp.where(iota(shape, 1) == wanted(iota(shape, 0)), 1.0, 0.0).astype(bf16)


def dot(a, b):
    return jnp.dot(a, b, preferred_element_type=f32)


def dot_t(a, b):
    return lax.dot_general(a, b, ROWS_BY_ROWS, preferred_element_type=f32)


def in_two(v):
    high = v.astype(bf16).astype(f32)
    return high, (v - high).astype(bf16).astype(f32)


def packed_stats(mh, ml, total):
    lh, ll = in_two(total)
    row = iota((8, mh.shape[1]), 0)
    out = jnp.where(row == 0, mh, jnp.where(row == 1, ml, jnp.where(row == 2, lh, ll)))
    return jnp.where(row < 4, out, 0.0).astype(bf16)


def stats_of(block):
    st = block[128:TALL, :].astype(f32)
    return st[0:1] + st[1:2], st[2:3] + st[3:4]


def merged(blocks):
    stats = [stats_of(b) for b in blocks]
    top = functools.reduce(jnp.maximum, [m for m, _ in stats])
    out, total = 0.0, 0.0
    for b, (m, l) in zip(blocks, stats):
        w = jnp.exp2(m - top)
        out = out + b[0:128, :].astype(f32) * w
        total = total + l * w
    return out, top, total


def kernel(
    len_ref, q_hbm, k_hbm, v_hbm, sk_hbm, sv_hbm, out_ref,
    qin, kvin, sk, sv, kv, kvs, qy, qs, qsuf, xs, r1, sx, ys, r2,
    so, sm, sl, local_sem, send_sem, recv_sem,
):
    x, y, z, c = place()
    loads = [
        pltpu.make_async_copy(src, dst, local_sem.at[i])
        for i, (src, dst) in enumerate(
            [(k_hbm, kvin.at[0]), (v_hbm, kvin.at[1]), (q_hbm, qin), (sk_hbm, sk), (sv_hbm, sv)]
        )
    ]
    for load in loads:
        load.start()

    peers = [dict(dx=d, e=e) for d in (1, 3) for e in (0, 1)] + [dict(e=1)]
    peers += [dict(dy=d, e=e) for d in (1, 2, 3) for e in (0, 1)]
    peers += [dict(dz=d, e=e) for d in range(1, 8) for e in (0, 1)]
    barrier = pltpu.get_barrier_semaphore()
    for p in peers:
        pl.semaphore_signal(barrier, inc=1, device_id=device(**p), device_id_type=MESH)

    groups = []

    def send(group, src, dst, sem=None, **to):
        pltpu.make_async_remote_copy(
            src_ref=src, dst_ref=dst, send_sem=send_sem.at[group],
            recv_sem=recv_sem.at[group if sem is None else sem],
            device_id=device(**to), device_id_type=MESH,
        ).start()

    def new_group(arrivals):
        groups.append(arrivals)
        return len(groups) - 1

    def wait_for(sem, ref):
        pltpu.make_async_copy(ref, ref, sem).wait()

    def arrived(group):
        wait_for(recv_sem.at[group], groups[group])

    def heads_of(k, last=None):
        return pl.ds(STARTS[k], sum(SIZES[k : (k if last is None else last) + 1]))

    def head_row(o):
        big = o // 16
        return (o % 16) * 16 + (big // 8 + c) % 2 * 8 + big % 8

    move = one_hot((256, 256), head_row)
    for t in range(2):
        loads[t].wait()
        for b in range(4):
            m = dot(move, kvin[t, 256 * b : 256 * b + 256, :]).astype(bf16).reshape(16, 16, 128)
            kv[t, :, 0, 16 * b : 16 * b + 16, :] = m[:8]
            kvs[t, :, 16 * b : 16 * b + 16, :] = m[8:]

    loads[2].wait()

    def query_row(o):
        e, g, j, r = o // 64, (o // 8) % 8, (o % 8) // 2, o % 2
        return j * 32 + ((e + c) % 2 * 8 + g) * 2 + r

    q = dot(one_hot((128, 128), query_row), qin[...]).astype(bf16)
    qsuf[...] = q
    qy[0, 0, 0] = q[:64].reshape(HEADS, 8, 128)
    qs[...] = q[64:].reshape(HEADS, 8, 128)

    pl.semaphore_wait(barrier, len(peers))

    kv_groups = [new_group(kv.at[:, heads_of(k), 1:8]) for k in range(CHUNKS)]

    def send_kv(k):
        h = heads_of(k)
        for dx, e in ((1, 0), (3, 1), (1, 1), (3, 0), (0, 1)):
            src = kvs.at[:, h] if e else kv.at[:, h, 0]
            relayed = {(1, 0): SEMS + k, (3, 1): SEMS + CHUNKS + k}.get((dx, e))
            send(kv_groups[k], src, kv.at[:, h, 2 * dx + e], sem=relayed, dx=dx, e=e)

    def forward_kv(k):
        h = heads_of(k)
        wait_for(recv_sem.at[SEMS + k], kv.at[:, h, 2])
        send(kv_groups[k], kv.at[:, h, 2], kv.at[:, h, 4], dx=1)
        wait_for(recv_sem.at[SEMS + CHUNKS + k], kv.at[:, h, 7])
        send(kv_groups[k], kv.at[:, h, 7], kv.at[:, h, 5], dx=3)

    def kv_arrived(k):
        wait_for(recv_sem.at[kv_groups[k]], kv.at[:, heads_of(k), 1:6])

    zy, yz = heads_of(1, EARLY - 1), heads_of(EARLY, CHUNKS - 1)

    def source(e, h):
        return qs.at[h] if e else qy.at[0, 0, 0, h]

    def send_q1(h, n):
        group = new_group(r2.at[1:16, 0:n])
        for dz in (4, 3, 5, 2, 6, 1, 7, 0):
            for e in (0, 1):
                if dz or e:
                    send(group, source(e, h), qy.at[0, dz, e, h], dz=dz, e=e)
        return group

    send_kv(0)
    q1a = send_q1(heads_of(0), SIZES[0])
    p1 = new_group(r2.at[1:8, 0 : HEADS - STARTS[EARLY]])
    for dy in (2, 1, 3, 0):
        for e in (0, 1):
            if dy or e:
                send(p1, source(e, yz), qy.at[dy, 0, e, yz], dy=dy, e=e)
    q1b = send_q1(zy, STARTS[EARLY] - STARTS[1])
    send_kv(1)
    send_kv(2)

    so[...] = jnp.zeros_like(so)
    sl[...] = jnp.zeros_like(sl)
    sm[...] = jnp.full_like(sm, HIDDEN)
    sx[...] = jnp.zeros_like(sx)
    loads[3].wait()
    loads[4].wait()
    length = len_ref[0]

    def suffix_piece(i, _):
        row, lane = iota((128, 128), 0), iota((128, 128), 1)
        head = (row // 64 + c) % 2 * 8 + (row // 8) % 8
        bias = jnp.where(lane % 16 == head, 0.0, HIDDEN)
        room = length - 3 + (row % 8) // 2 - lane // 16
        at = pl.ds(pl.multiple_of(i * PIECE, PIECE), PIECE)
        raw = dot_t(qsuf[...], sk[at, :])
        parts = []
        for t in range(PIECE // 128):
            part = raw[:, 128 * t : 128 * t + 128] * LOG2_SCALE + bias
            parts.append(jnp.where(room > i * (PIECE // 16) + 8 * t, part, HIDDEN))
        old = sm[...]
        top = jnp.maximum(old, jnp.max(functools.reduce(jnp.maximum, parts), 1, keepdims=True))
        weights = [jnp.exp2(part - top) for part in parts]
        shrink = jnp.exp2(old - top)
        sm[...] = top
        sl[...] = sl[...] * shrink + jnp.sum(functools.reduce(jnp.add, weights), 1, keepdims=True)
        rounded = jnp.concatenate([w.astype(bf16) for w in weights], axis=1)
        so[...] = so[...] * shrink + dot(rounded, sv[at, :])
        return 0

    def suffix(first, last):
        lax.fori_loop(first, last, suffix_piece, 0)

    q2 = {}

    def send_q_z(k):
        h = heads_of(k)
        q2[k] = new_group(qy.at[:, 1:8, :, h])
        for dz in (4, 3, 5, 2, 6, 1, 7):
            send(q2[k], qy.at[:, 0, :, h], qy.at[:, dz, :, h], dz=dz)

    def send_q_y(k):
        h = heads_of(k)
        q2[k] = new_group(qy.at[1:4, :, :, h])
        for dy in (2, 1, 3):
            send(q2[k], qy.at[0, :, :, h], qy.at[dy, :, :, h], dy=dy)

    suffix(0, 3)
    arrived(p1)
    for k in range(EARLY, CHUNKS):
        send_q_z(k)
    forward_kv(0)
    send_kv(3)
    arrived(q1a)
    send_q_y(0)
    suffix(3, 4)
    forward_kv(1)
    send_kv(4)
    arrived(q1b)
    for k in range(1, EARLY):
        send_q_y(k)
    suffix(4, 6)
    forward_kv(2)
    send_kv(5)
    suffix(6, 16384 // PIECE)
    forward_kv(3)
    send_kv(6)

    eye = one_hot((128, 128), lambda o: o)

    def prompt_head(g, _):
        keys = kv[0, g].reshape(512, 128)
        values = kv[1, g].reshape(512, 128)
        rows = qy[:, :, :, g].astype(f32).reshape(512, 128).astype(bf16)
        scores = dot_t(keys, rows) * LOG2_SCALE
        mh, ml = in_two(jnp.max(scores, 0, keepdims=True))
        weights = jnp.exp2(scores - (mh + ml))
        stats = packed_stats(mh, ml, jnp.sum(weights, 0, keepdims=True))
        out = dot(dot_t(eye, values).astype(bf16), weights.astype(bf16)).astype(bf16)
        for dy in range(4):
            xs[dy, g, 0:128, :] = out[:, 128 * dy : 128 * dy + 128]
            xs[dy, g, 128:TALL, :] = stats[:, 128 * dy : 128 * dy + 128]
        return 0

    rs1 = []
    rs2 = []

    def over_y(k):
        arrived(rs1[k])
        first, n = tile_of(STARTS[k]), SIZES[k]
        for i in range(n):
            g = STARTS[k] + i
            out, top, total = merged([xs[0, g]] + [r1[dy, g] for dy in range(1, 4)])
            mh, ml = in_two(top)
            adjust = jnp.exp2(top - (mh + ml))
            ys[:, first + i] = dot_t(eye, (out * adjust).astype(bf16)).astype(bf16).reshape(16, 8, 128)
            sx[TAILS.index(LAST[k]), 16 * g : 16 * g + 8, :] = packed_stats(mh, ml, total * adjust)
        if k in TAILS:
            stats = dot_t(eye, sx[TAILS.index(k)]).astype(bf16)
            ys[:, first + n] = stats.reshape(16, 8, 128)
            n += 1
        t = pl.ds(first, n)
        rs2.append(new_group(r2.at[1:16, t]))
        for dz in (4, 3, 5, 2, 6, 1, 7, 0):
            for e in (0, 1):
                if dz or e:
                    send(rs2[k], ys.at[2 * dz + e, t], r2.at[2 * dz + e, t], dz=8 - dz, e=e)

    def prompt(k):
        arrived(q2[k])
        kv_arrived(k)
        lax.fori_loop(STARTS[k], STARTS[k] + SIZES[k], prompt_head, 0)
        h = heads_of(k)
        rs1.append(new_group(r1.at[1:4, h]))
        for dy in (2, 1, 3):
            send(rs1[k], xs.at[dy, h], r1.at[dy, h], dy=4 - dy)

    prompt(0)
    forward_kv(4)
    send_kv(7)
    prompt(1)
    prompt(2)
    forward_kv(5)
    prompt(3)
    over_y(0)
    forward_kv(6)
    prompt(4)
    over_y(1)
    forward_kv(7)
    prompt(5)
    over_y(2)
    prompt(6)
    over_y(3)
    prompt(7)
    for k in range(4, CHUNKS):
        over_y(k)

    begun = 0
    for tail in TAILS:
        mine = range(begun, tail + 1)
        begun = tail + 1
        for k in mine:
            arrived(rs2[k])
        heads = range(STARTS[mine[0]], STARTS[tail] + SIZES[tail])
        at_stats = tile_of(heads[-1]) + 1
        for e in (0, 1):
            blocks = [r2.at[2 * dz + e] if dz or e else ys.at[0] for dz in range(8)]
            lane = iota((8, 128), 1)
            top_own = total_own = jnp.zeros((8, 128), f32)
            for g in heads:
                at = (e * 8 + g) * 8
                top_own = jnp.where(lane // 16 == g, sm[at : at + 8, :], top_own)
                total_own = jnp.where(lane // 16 == g, sl[at : at + 8, :], total_own)
            tiles = [b[at_stats].astype(f32) for b in blocks]
            tops = [t + pltpu.roll(t, 127, 1) for t in tiles] + [top_own]
            totals = [pltpu.roll(t, 126, 1) + pltpu.roll(t, 125, 1) for t in tiles] + [total_own]
            top = functools.reduce(jnp.maximum, tops)
            factors = [jnp.exp2(t - top) for t in tops]
            whole = functools.reduce(jnp.add, [f * t for f, t in zip(factors, totals)])
            factors = [f / whole for f in factors]
            for g in heads:
                at = (e * 8 + g) * 8
                parts = [b[tile_of(g)].astype(f32) for b in blocks] + [so[at : at + 8, :]]
                so[at : at + 8, :] = functools.reduce(
                    jnp.add, [p * f[:, 16 * g : 16 * g + 1] for p, f in zip(parts, factors)]
                )

    def final_row(o):
        j, g, r = o // 32, (o // 2) % 16, o % 2
        return (g // 8 + c) % 2 * 64 + g % 8 * 8 + j * 2 + r

    out_ref[...] = dot(one_hot((128, 128), final_row), so[...].astype(bf16)).astype(bf16)
    for group, arrivals in enumerate(groups):
        wait_for(send_sem.at[group], arrivals)


def body(queries, prefix_keys, prefix_values, suffix_keys, suffix_values, lengths):
    vmem, anyspace = pltpu.VMEM, pl.BlockSpec(memory_space=pltpu.HBM)
    out = pl.pallas_call(
        kernel,
        name="attend",
        out_shape=jax.ShapeDtypeStruct((128, 128), bf16),
        in_specs=[pl.BlockSpec(memory_space=pltpu.SMEM)] + [anyspace] * 5,
        out_specs=pl.BlockSpec(memory_space=vmem),
        scratch_shapes=[
            vmem((128, 128), bf16),
            vmem((2, 1024, 128), bf16),
            vmem((16384, 128), bf16),
            vmem((16384, 128), bf16),
            vmem((2, HEADS, 8, 64, 128), bf16),
            vmem((2, HEADS, 64, 128), bf16),
            vmem((4, 8, 2, HEADS, 8, 128), bf16),
            vmem((HEADS, 8, 128), bf16),
            vmem((128, 128), bf16),
            vmem((4, HEADS, TALL, 128), bf16),
            vmem((4, HEADS, TALL, 128), bf16),
            vmem((len(TAILS), 128, 128), bf16),
            vmem((16, TILES, 8, 128), bf16),
            vmem((16, TILES, 8, 128), bf16),
            vmem((128, 128), f32),
            vmem((128, 128), f32),
            vmem((128, 128), f32),
            pltpu.SemaphoreType.DMA((5,)),
            pltpu.SemaphoreType.DMA((SEMS,)),
            pltpu.SemaphoreType.DMA((SEMS + 2 * CHUNKS,)),
        ],
        compiler_params=pltpu.CompilerParams(
            collective_id=0, has_side_effects=True, vmem_limit_bytes=67_043_328
        ),
    )(
        lengths,
        queries.reshape(128, 128),
        prefix_keys.reshape(1024, 128),
        prefix_values.reshape(1024, 128),
        suffix_keys.reshape(16384, 128),
        suffix_values.reshape(16384, 128),
    )
    return out.reshape(1, 4, 32, 128)


def solution(mesh):
    return jax.shard_map(
        body,
        mesh=mesh,
        in_specs=(
            P(("kv", "batch"), None, None, None),
            P(("kv", "batch"), None, None),
            P(("kv", "batch"), None, None),
            P(("kv", "batch"), None, None, None),
            P(("kv", "batch"), None, None, None),
            P(("kv", "batch")),
        ),
        out_specs=P(("kv", "batch"), None, None, None),
        check_vma=False,
    )
```

```python
import functools
import math

import jax
import jax.numpy as jnp
from jax import lax
from jax.experimental import pallas as pl
from jax.experimental.pallas import tpu as pltpu
from jax.sharding import PartitionSpec as P

QUERY_SCALE = 144
LOG2_SCALE = QUERY_SCALE ** (-0.5) * math.log2(math.e)
HIDDEN = -1e30

HEADS = 8
SIZES = (1,) * HEADS
STARTS = tuple(sum(SIZES[:k]) for k in range(len(SIZES)))
CHUNKS = len(SIZES)
EARLY = 4
LAST = (3,) * 4 + (7,) * 4
TAILS = tuple(sorted(set(LAST)))


def tile_of(head):
    return head + sum(STARTS[t] + SIZES[t] <= head for t in TAILS)


TILES = HEADS + len(TAILS)
SEMS = 3 + 4 * CHUNKS
TALL = 136
PIECE = 2048

f32, bf16 = jnp.float32, jnp.bfloat16
MESH = pl.DeviceIdType.MESH
ROWS_BY_ROWS = (((1,), (1,)), ((), ()))


def place():
    kv, b = lax.axis_index("kv"), lax.axis_index("batch")
    return b % 4, (b // 4) * 2 + (kv // 2) % 2, kv // 4, kv % 2


def device(dx=0, dy=0, dz=0, e=0):
    x, y, z, c = place()
    x, y, z = (x + dx) % 4, (y + dy) % 4, (z + dz) % 8
    c = (c + e) % 2
    return (z * 2 + y % 2) * 2 + c, (y // 2) * 4 + x


def iota(shape, dim):
    return lax.broadcasted_iota(jnp.int32, shape, dim)


def one_hot(shape, wanted):
    return jnp.where(iota(shape, 1) == wanted(iota(shape, 0)), 1.0, 0.0).astype(bf16)


def dot(a, b):
    return jnp.dot(a, b, preferred_element_type=f32)


def dot_t(a, b):
    return lax.dot_general(a, b, ROWS_BY_ROWS, preferred_element_type=f32)


def in_two(v):
    high = v.astype(bf16).astype(f32)
    return high, (v - high).astype(bf16).astype(f32)


def packed_stats(mh, ml, total):
    lh, ll = in_two(total)
    row = iota((8, mh.shape[1]), 0)
    out = jnp.where(row == 0, mh, jnp.where(row == 1, ml, jnp.where(row == 2, lh, ll)))
    return jnp.where(row < 4, out, 0.0).astype(bf16)


def stats_of(block):
    st = block[128:TALL, :].astype(f32)
    return st[0:1] + st[1:2], st[2:3] + st[3:4]


def merged(blocks):
    stats = [stats_of(b) for b in blocks]
    top = functools.reduce(jnp.maximum, [m for m, _ in stats])
    out, total = 0.0, 0.0
    for b, (m, l) in zip(blocks, stats):
        w = jnp.exp2(m - top)
        out = out + b[0:128, :].astype(f32) * w
        total = total + l * w
    return out, top, total


def kernel(
    len_hbm, q_hbm, k_hbm, v_hbm, sk_hbm, sv_hbm, out_ref,
    qin, kvin, sk, sv, kv, kvs, qy, qs, qsuf, xs, r1, sx, ys, r2,
    so, sm, sl, len_ref, local_sem, send_sem, recv_sem,
):
    x, y, z, c = place()
    loads = [
        pltpu.make_async_copy(src, dst, local_sem.at[i])
        for i, (src, dst) in enumerate(
            [(k_hbm, kvin.at[0]), (v_hbm, kvin.at[1]), (q_hbm, qin), (len_hbm, len_ref), (sk_hbm, sk), (sv_hbm, sv)]
        )
    ]
    for load in loads:
        load.start()

    peers = [dict(dx=d, e=e) for d in (1, 3) for e in (0, 1)] + [dict(e=1)]
    peers += [dict(dy=d, e=e) for d in (1, 2, 3) for e in (0, 1)]
    peers += [dict(dz=d, e=e) for d in range(1, 8) for e in (0, 1)]
    barrier = pltpu.get_barrier_semaphore()
    for p in peers:
        pl.semaphore_signal(barrier, inc=1, device_id=device(**p), device_id_type=MESH)

    groups = []

    def send(group, src, dst, sem=None, **to):
        pltpu.make_async_remote_copy(
            src_ref=src, dst_ref=dst, send_sem=send_sem,
            recv_sem=recv_sem.at[group if sem is None else sem],
            device_id=device(**to), device_id_type=MESH,
        ).start()

    def new_group(arrivals):
        groups.append(arrivals)
        return len(groups) - 1

    def wait_for(sem, ref):
        pltpu.make_async_copy(ref, ref, sem).wait()

    def arrived(group):
        wait_for(recv_sem.at[group], groups[group])

    def heads_of(k, last=None):
        return pl.ds(STARTS[k], sum(SIZES[k : (k if last is None else last) + 1]))

    def head_row(o):
        big = o // 16
        return (o % 16) * 16 + (big // 8 + c) % 2 * 8 + big % 8

    move = one_hot((256, 256), head_row)
    for t in range(2):
        loads[t].wait()
        for b in range(4):
            m = dot(move, kvin[t, 256 * b : 256 * b + 256, :]).astype(bf16).reshape(16, 16, 128)
            kv[t, :, 0, 16 * b : 16 * b + 16, :] = m[:8]
            kvs[t, :, 16 * b : 16 * b + 16, :] = m[8:]

    pl.semaphore_wait(barrier, len(peers))

    kv_groups = [new_group(kv.at[:, heads_of(k), 1:8]) for k in range(CHUNKS)]

    def send_kv(k):
        h = heads_of(k)
        for dx, e in ((1, 0), (3, 1), (1, 1), (3, 0), (0, 1)):
            src = kvs.at[:, h] if e else kv.at[:, h, 0]
            relayed = SEMS + k if (dx, e) in ((1, 0), (3, 1)) else None
            send(kv_groups[k], src, kv.at[:, h, 2 * dx + e], sem=relayed, dx=dx, e=e)

    def forward_kv(k):
        h = heads_of(k)
        wait_for(recv_sem.at[SEMS + k], kv.at[:, h, 2:4])
        send(kv_groups[k], kv.at[:, h, 2], kv.at[:, h, 4], dx=1)
        send(kv_groups[k], kv.at[:, h, 7], kv.at[:, h, 5], dx=3)

    def kv_arrived(k):
        wait_for(recv_sem.at[kv_groups[k]], kv.at[:, heads_of(k), 1:6])

    zy, yz = heads_of(1, EARLY - 1), heads_of(EARLY, CHUNKS - 1)

    def source(e, h):
        return qs.at[h] if e else qy.at[0, 0, 0, h]

    def send_q1(h, n):
        group = new_group(r2.at[1:16, 0:n])
        for dz in (4, 3, 5, 2, 6, 1, 7, 0):
            for e in (0, 1):
                if dz or e:
                    send(group, source(e, h), qy.at[0, dz, e, h], dz=dz, e=e)
        return group

    send_kv(0)
    loads[2].wait()

    def query_row(o):
        e, g, j, r = o // 64, (o // 8) % 8, (o % 8) // 2, o % 2
        return j * 32 + ((e + c) % 2 * 8 + g) * 2 + r

    q = dot(one_hot((128, 128), query_row), qin[...]).astype(bf16)
    qsuf[...] = q
    qy[0, 0, 0] = q[:64].reshape(HEADS, 8, 128)
    qs[...] = q[64:].reshape(HEADS, 8, 128)

    q1a = send_q1(heads_of(0), SIZES[0])
    p1 = new_group(r2.at[1:8, 0 : HEADS - STARTS[EARLY]])
    for dy in (2, 1, 3, 0):
        for e in (0, 1):
            if dy or e:
                send(p1, source(e, yz), qy.at[dy, 0, e, yz], dy=dy, e=e)
    q1b = send_q1(zy, STARTS[EARLY] - STARTS[1])
    send_kv(1)
    send_kv(2)

    so[...] = jnp.zeros_like(so)
    sl[...] = jnp.zeros_like(sl)
    sm[...] = jnp.full_like(sm, HIDDEN)
    sx[...] = jnp.zeros_like(sx)
    for load in loads[3:]:
        load.wait()
    length = len_ref[0]

    def suffix_piece(i, _):
        row, lane = iota((128, 128), 0), iota((128, 128), 1)
        head = (row // 64 + c) % 2 * 8 + (row // 8) % 8
        bias = jnp.where(lane % 16 == head, 0.0, HIDDEN)
        room = length - 3 + (row % 8) // 2 - lane // 16
        at = pl.ds(pl.multiple_of(i * PIECE, PIECE), PIECE)
        raw = dot_t(qsuf[...], sk[at, :])
        parts = []
        for t in range(PIECE // 128):
            part = raw[:, 128 * t : 128 * t + 128] * LOG2_SCALE + bias
            parts.append(jnp.where(room > i * (PIECE // 16) + 8 * t, part, HIDDEN))
        old = sm[...]
        top = jnp.maximum(old, jnp.max(functools.reduce(jnp.maximum, parts), 1, keepdims=True))
        weights = [jnp.exp2(part - top) for part in parts]
        shrink = jnp.exp2(old - top)
        sm[...] = top
        sl[...] = sl[...] * shrink + jnp.sum(functools.reduce(jnp.add, weights), 1, keepdims=True)
        rounded = jnp.concatenate([w.astype(bf16) for w in weights], axis=1)
        so[...] = so[...] * shrink + dot(rounded, sv[at, :])
        return 0

    def suffix(first, last):
        lax.fori_loop(first, last, suffix_piece, 0)

    q2 = {}

    def send_q_z(k):
        h = heads_of(k)
        q2[k] = new_group(qy.at[:, 1:8, :, h])
        for dz in (4, 3, 5, 2, 6, 1, 7):
            send(q2[k], qy.at[:, 0, :, h], qy.at[:, dz, :, h], dz=dz)

    def send_q_y(k):
        h = heads_of(k)
        q2[k] = new_group(qy.at[1:4, :, :, h])
        for dy in (2, 1, 3):
            send(q2[k], qy.at[0, :, :, h], qy.at[dy, :, :, h], dy=dy)

    suffix(0, 3)
    forward_kv(0)
    send_kv(3)
    arrived(p1)
    for k in range(EARLY, CHUNKS):
        send_q_z(k)
    arrived(q1a)
    send_q_y(0)
    forward_kv(1)
    send_kv(4)
    arrived(q1b)
    for k in range(1, EARLY):
        send_q_y(k)
    suffix(3, 4)
    forward_kv(2)
    send_kv(5)
    suffix(4, 5)
    forward_kv(3)
    send_kv(6)

    eye = one_hot((128, 128), lambda o: o)

    def prompt_head(g, _):
        keys = kv[0, g].reshape(512, 128)
        values = kv[1, g].reshape(512, 128)
        rows = qy[:, :, :, g].astype(f32).reshape(512, 128).astype(bf16)
        scores = dot_t(keys, rows) * LOG2_SCALE
        mh, ml = in_two(jnp.max(scores, 0, keepdims=True))
        weights = jnp.exp2(scores - (mh + ml))
        stats = packed_stats(mh, ml, jnp.sum(weights, 0, keepdims=True))
        out = dot(dot_t(eye, values).astype(bf16), weights.astype(bf16)).astype(bf16)
        for dy in range(4):
            xs[dy, g, 0:128, :] = out[:, 128 * dy : 128 * dy + 128]
            xs[dy, g, 128:TALL, :] = stats[:, 128 * dy : 128 * dy + 128]
        return 0

    rs1 = []
    rs2 = []

    def over_y(k):
        arrived(rs1[k])
        first, n = tile_of(STARTS[k]), SIZES[k]
        for i in range(n):
            g = STARTS[k] + i
            out, top, total = merged([xs[0, g]] + [r1[dy, g] for dy in range(1, 4)])
            mh, ml = in_two(top)
            adjust = jnp.exp2(top - (mh + ml))
            ys[:, first + i] = dot_t(eye, (out * adjust).astype(bf16)).astype(bf16).reshape(16, 8, 128)
            sx[TAILS.index(LAST[k]), 16 * g : 16 * g + 8, :] = packed_stats(mh, ml, total * adjust)
        if k in TAILS:
            stats = dot_t(eye, sx[TAILS.index(k)]).astype(bf16)
            ys[:, first + n] = stats.reshape(16, 8, 128)
            n += 1
        t = pl.ds(first, n)
        rs2.append(new_group(r2.at[1:16, t]))
        for dz in (4, 3, 5, 2, 6, 1, 7, 0):
            for e in (0, 1):
                if dz or e:
                    send(rs2[k], ys.at[2 * dz + e, t], r2.at[2 * dz + e, t], dz=8 - dz, e=e)

    def prompt(k):
        arrived(q2[k])
        kv_arrived(k)
        lax.fori_loop(STARTS[k], STARTS[k] + SIZES[k], prompt_head, 0)
        h = heads_of(k)
        rs1.append(new_group(r1.at[1:4, h]))
        for dy in (2, 1, 3):
            send(rs1[k], xs.at[dy, h], r1.at[dy, h], dy=4 - dy)

    prompt(0)
    forward_kv(4)
    send_kv(7)
    prompt(1)
    prompt(2)
    forward_kv(5)
    prompt(3)
    over_y(0)
    forward_kv(6)
    prompt(4)
    over_y(1)
    forward_kv(7)
    prompt(5)
    over_y(2)
    prompt(6)
    over_y(3)
    prompt(7)
    for k in range(4, CHUNKS):
        over_y(k)
    suffix(5, 16384 // PIECE)

    begun = 0
    for tail in TAILS:
        mine = range(begun, tail + 1)
        begun = tail + 1
        for k in mine:
            arrived(rs2[k])
        heads = range(STARTS[mine[0]], STARTS[tail] + SIZES[tail])
        at_stats = tile_of(heads[-1]) + 1
        for e in (0, 1):
            blocks = [r2.at[2 * dz + e] if dz or e else ys.at[0] for dz in range(8)]
            lane = iota((8, 128), 1)
            top_own = total_own = jnp.zeros((8, 128), f32)
            for g in heads:
                at = (e * 8 + g) * 8
                top_own = jnp.where(lane // 16 == g, sm[at : at + 8, :], top_own)
                total_own = jnp.where(lane // 16 == g, sl[at : at + 8, :], total_own)
            tiles = [b[at_stats].astype(f32) for b in blocks]
            tops = [t + pltpu.roll(t, 127, 1) for t in tiles] + [top_own]
            totals = [pltpu.roll(t, 126, 1) + pltpu.roll(t, 125, 1) for t in tiles] + [total_own]
            top = functools.reduce(jnp.maximum, tops)
            factors = [jnp.exp2(t - top) for t in tops]
            whole = functools.reduce(jnp.add, [f * t for f, t in zip(factors, totals)])
            factors = [f / whole for f in factors]
            for g in heads:
                at = (e * 8 + g) * 8
                parts = [b[tile_of(g)].astype(f32) for b in blocks] + [so[at : at + 8, :]]
                so[at : at + 8, :] = functools.reduce(
                    jnp.add, [p * f[:, 16 * g : 16 * g + 1] for p, f in zip(parts, factors)]
                )

    def final_row(o):
        j, g, r = o // 32, (o // 2) % 16, o % 2
        return (g // 8 + c) % 2 * 64 + g % 8 * 8 + j * 2 + r

    out_ref[...] = dot(one_hot((128, 128), final_row), so[...].astype(bf16)).astype(bf16)
    sent = sum(math.prod(arrivals.shape) for arrivals in groups)
    wait_for(send_sem, sk.at[0 : sent // 128])


def body(queries, prefix_keys, prefix_values, suffix_keys, suffix_values, lengths):
    vmem, anyspace = pltpu.VMEM, pl.BlockSpec(memory_space=pltpu.HBM)
    out = pl.pallas_call(
        kernel,
        name="attend",
        out_shape=jax.ShapeDtypeStruct((128, 128), bf16),
        in_specs=[anyspace] * 6,
        out_specs=pl.BlockSpec(memory_space=vmem),
        scratch_shapes=[
            vmem((128, 128), bf16),
            vmem((2, 1024, 128), bf16),
            vmem((16384, 128), bf16),
            vmem((16384, 128), bf16),
            vmem((2, HEADS, 8, 64, 128), bf16),
            vmem((2, HEADS, 64, 128), bf16),
            vmem((4, 8, 2, HEADS, 8, 128), bf16),
            vmem((HEADS, 8, 128), bf16),
            vmem((128, 128), bf16),
            vmem((4, HEADS, TALL, 128), bf16),
            vmem((4, HEADS, TALL, 128), bf16),
            vmem((len(TAILS), 128, 128), bf16),
            vmem((16, TILES, 8, 128), bf16),
            vmem((16, TILES, 8, 128), bf16),
            vmem((128, 128), f32),
            vmem((128, 128), f32),
            vmem((128, 128), f32),
            pltpu.SMEM((1,), jnp.int32),
            pltpu.SemaphoreType.DMA((6,)),
            pltpu.SemaphoreType.DMA,
            pltpu.SemaphoreType.DMA((SEMS + CHUNKS,)),
        ],
        compiler_params=pltpu.CompilerParams(
            collective_id=0, has_side_effects=True, vmem_limit_bytes=67_043_328
        ),
    )(
        lengths,
        queries.reshape(128, 128),
        prefix_keys.reshape(1024, 128),
        prefix_values.reshape(1024, 128),
        suffix_keys.reshape(16384, 128),
        suffix_values.reshape(16384, 128),
    )
    return out.reshape(1, 4, 32, 128)


def solution(mesh):
    return jax.shard_map(
        body,
        mesh=mesh,
        in_specs=(
            P(("kv", "batch"), None, None, None),
            P(("kv", "batch"), None, None),
            P(("kv", "batch"), None, None),
            P(("kv", "batch"), None, None, None),
            P(("kv", "batch"), None, None, None),
            P(("kv", "batch")),
        ),
        out_specs=P(("kv", "batch"), None, None, None),
        check_vma=False,
    )
```

```python
import functools
import math

import jax
import jax.numpy as jnp
from jax import lax
from jax.experimental import pallas as pl
from jax.experimental.pallas import tpu as pltpu
from jax.sharding import PartitionSpec as P

QUERY_SCALE = 144
LOG2_SCALE = QUERY_SCALE ** (-0.5) * math.log2(math.e)
HIDDEN = -1e30

HEADS = 8
SIZES = (1,) * HEADS
STARTS = tuple(sum(SIZES[:k]) for k in range(len(SIZES)))
CHUNKS = len(SIZES)
EARLY = 4
LAST = (3,) * 4 + (7,) * 4
TAILS = tuple(sorted(set(LAST)))


def tile_of(head):
    return head + sum(STARTS[t] + SIZES[t] <= head for t in TAILS)


TILES = HEADS + len(TAILS)
SEMS = 3 + 4 * CHUNKS
TALL = 136
PIECE = 2048

f32, bf16 = jnp.float32, jnp.bfloat16
MESH = pl.DeviceIdType.MESH
ROWS_BY_ROWS = (((1,), (1,)), ((), ()))


def place():
    kv, b = lax.axis_index("kv"), lax.axis_index("batch")
    return b % 4, (b // 4) * 2 + (kv // 2) % 2, kv // 4, kv % 2


def device(dx=0, dy=0, dz=0, e=0):
    x, y, z, c = place()
    x, y, z = (x + dx) % 4, (y + dy) % 4, (z + dz) % 8
    c = (c + e) % 2
    return (z * 2 + y % 2) * 2 + c, (y // 2) * 4 + x


def iota(shape, dim):
    return lax.broadcasted_iota(jnp.int32, shape, dim)


def one_hot(shape, wanted):
    return jnp.where(iota(shape, 1) == wanted(iota(shape, 0)), 1.0, 0.0).astype(bf16)


def dot(a, b):
    return jnp.dot(a, b, preferred_element_type=f32)


def dot_t(a, b):
    return lax.dot_general(a, b, ROWS_BY_ROWS, preferred_element_type=f32)


def in_two(v):
    high = v.astype(bf16).astype(f32)
    return high, (v - high).astype(bf16).astype(f32)


def packed_stats(mh, ml, total):
    lh, ll = in_two(total)
    row = iota((8, mh.shape[1]), 0)
    out = jnp.where(row == 0, mh, jnp.where(row == 1, ml, jnp.where(row == 2, lh, ll)))
    return jnp.where(row < 4, out, 0.0).astype(bf16)


def stats_of(block):
    st = block[128:TALL, :].astype(f32)
    return st[0:1] + st[1:2], st[2:3] + st[3:4]


def merged(blocks):
    stats = [stats_of(b) for b in blocks]
    top = functools.reduce(jnp.maximum, [m for m, _ in stats])
    out, total = 0.0, 0.0
    for b, (m, l) in zip(blocks, stats):
        w = jnp.exp2(m - top)
        out = out + b[0:128, :].astype(f32) * w
        total = total + l * w
    return out, top, total


def kernel(
    len_hbm, q_hbm, k_hbm, v_hbm, sk_hbm, sv_hbm, out_ref,
    qin, kvin, sk, sv, kv, kvs, qy, qs, qsuf, xs, r1, sx, ys, r2,
    so, sm, sl, len_ref, local_sem, send_sem, recv_sem,
):
    x, y, z, c = place()
    loads = [
        pltpu.make_async_copy(src, dst, local_sem.at[i])
        for i, (src, dst) in enumerate(
            [(k_hbm, kvin.at[0]), (v_hbm, kvin.at[1]), (q_hbm, qin), (len_hbm, len_ref), (sk_hbm, sk), (sv_hbm, sv)]
        )
    ]
    for load in loads:
        load.start()

    peers = [dict(dx=d, e=e) for d in (1, 3) for e in (0, 1)] + [dict(e=1)]
    peers += [dict(dy=d, e=e) for d in (1, 2, 3) for e in (0, 1)]
    peers += [dict(dz=d, e=e) for d in range(1, 8) for e in (0, 1)]
    barrier = pltpu.get_barrier_semaphore()
    for p in peers:
        pl.semaphore_signal(barrier, inc=1, device_id=device(**p), device_id_type=MESH)

    groups = []

    def send(group, src, dst, sem=None, **to):
        pltpu.make_async_remote_copy(
            src_ref=src, dst_ref=dst, send_sem=send_sem,
            recv_sem=recv_sem.at[group if sem is None else sem],
            device_id=device(**to), device_id_type=MESH,
        ).start()

    def new_group(arrivals):
        groups.append(arrivals)
        return len(groups) - 1

    def wait_for(sem, ref):
        pltpu.make_async_copy(ref, ref, sem).wait()

    def arrived(group):
        wait_for(recv_sem.at[group], groups[group])

    def heads_of(k, last=None):
        return pl.ds(STARTS[k], sum(SIZES[k : (k if last is None else last) + 1]))

    def head_row(o):
        big = o // 16
        return (o % 16) * 16 + (big // 8 + c) % 2 * 8 + big % 8

    move = one_hot((256, 256), head_row)
    for t in range(2):
        loads[t].wait()
        for b in range(4):
            m = dot(move, kvin[t, 256 * b : 256 * b + 256, :]).astype(bf16).reshape(16, 16, 128)
            kv[t, :, 0, 16 * b : 16 * b + 16, :] = m[:8]
            kvs[t, :, 16 * b : 16 * b + 16, :] = m[8:]

    pl.semaphore_wait(barrier, len(peers))

    kv_groups = [new_group(kv.at[:, heads_of(k), 1:8]) for k in range(CHUNKS)]

    def send_kv(k):
        h = heads_of(k)
        for dx, e in ((1, 0), (3, 1), (1, 1), (3, 0), (0, 1)):
            src = kvs.at[:, h] if e else kv.at[:, h, 0]
            relayed = SEMS + k if (dx, e) in ((1, 0), (3, 1)) else None
            send(kv_groups[k], src, kv.at[:, h, 2 * dx + e], sem=relayed, dx=dx, e=e)

    def forward_kv(k):
        h = heads_of(k)
        wait_for(recv_sem.at[SEMS + k], kv.at[:, h, 2:4])
        send(kv_groups[k], kv.at[:, h, 2], kv.at[:, h, 4], dx=1)
        send(kv_groups[k], kv.at[:, h, 7], kv.at[:, h, 5], dx=3)

    def kv_arrived(k):
        wait_for(recv_sem.at[kv_groups[k]], kv.at[:, heads_of(k), 1:6])

    zy, yz = heads_of(1, EARLY - 1), heads_of(EARLY, CHUNKS - 1)

    def source(e, h):
        return qs.at[h] if e else qy.at[0, 0, 0, h]

    def send_q1(h, n):
        group = new_group(r2.at[1:16, 0:n])
        for dz in (4, 3, 5, 2, 6, 1, 7, 0):
            for e in (0, 1):
                if dz or e:
                    send(group, source(e, h), qy.at[0, dz, e, h], dz=dz, e=e)
        return group

    send_kv(0)
    loads[2].wait()

    def query_row(o):
        e, g, j, r = o // 64, (o // 8) % 8, (o % 8) // 2, o % 2
        return j * 32 + ((e + c) % 2 * 8 + g) * 2 + r

    q = dot(one_hot((128, 128), query_row), qin[...]).astype(bf16)
    qsuf[...] = q
    qy[0, 0, 0] = q[:64].reshape(HEADS, 8, 128)
    qs[...] = q[64:].reshape(HEADS, 8, 128)

    q1a = send_q1(heads_of(0), SIZES[0])
    p1 = new_group(r2.at[1:8, 0 : HEADS - STARTS[EARLY]])
    for dy in (2, 1, 3, 0):
        for e in (0, 1):
            if dy or e:
                send(p1, source(e, yz), qy.at[dy, 0, e, yz], dy=dy, e=e)
    q1b = send_q1(zy, STARTS[EARLY] - STARTS[1])
    send_kv(1)
    send_kv(2)

    so[...] = jnp.zeros_like(so)
    sl[...] = jnp.zeros_like(sl)
    sm[...] = jnp.full_like(sm, HIDDEN)
    sx[...] = jnp.zeros_like(sx)
    for load in loads[3:]:
        load.wait()
    length = len_ref[0]

    def suffix_piece(i, _):
        row, lane = iota((128, 128), 0), iota((128, 128), 1)
        head = (row // 64 + c) % 2 * 8 + (row // 8) % 8
        bias = jnp.where(lane % 16 == head, 0.0, HIDDEN)
        room = length - 3 + (row % 8) // 2 - lane // 16
        at = pl.ds(pl.multiple_of(i * PIECE, PIECE), PIECE)
        raw = dot_t(qsuf[...], sk[at, :])
        parts = []
        for t in range(PIECE // 128):
            part = raw[:, 128 * t : 128 * t + 128] * LOG2_SCALE + bias
            parts.append(jnp.where(room > i * (PIECE // 16) + 8 * t, part, HIDDEN))
        old = sm[...]
        top = jnp.maximum(old, jnp.max(functools.reduce(jnp.maximum, parts), 1, keepdims=True))
        weights = [jnp.exp2(part - top) for part in parts]
        shrink = jnp.exp2(old - top)
        sm[...] = top
        sl[...] = sl[...] * shrink + jnp.sum(functools.reduce(jnp.add, weights), 1, keepdims=True)
        rounded = jnp.concatenate([w.astype(bf16) for w in weights], axis=1)
        so[...] = so[...] * shrink + dot(rounded, sv[at, :])
        return 0

    def suffix(first, last):
        lax.fori_loop(first, last, suffix_piece, 0)

    q2 = {}

    def send_q_z(k):
        h = heads_of(k)
        q2[k] = new_group(qy.at[:, 1:8, :, h])
        for dz in (4, 3, 5, 2, 6, 1, 7):
            send(q2[k], qy.at[:, 0, :, h], qy.at[:, dz, :, h], dz=dz)

    def send_q_y(k):
        h = heads_of(k)
        q2[k] = new_group(qy.at[1:4, :, :, h])
        for dy in (2, 1, 3):
            send(q2[k], qy.at[0, :, :, h], qy.at[dy, :, :, h], dy=dy)

    suffix(0, 3)
    forward_kv(0)
    send_kv(3)
    arrived(p1)
    for k in range(EARLY, CHUNKS):
        send_q_z(k)
    arrived(q1a)
    send_q_y(0)
    forward_kv(1)
    send_kv(4)
    arrived(q1b)
    for k in range(1, EARLY):
        send_q_y(k)
    suffix(3, 4)
    forward_kv(2)
    send_kv(5)
    suffix(4, 5)
    forward_kv(3)
    send_kv(6)
    send_kv(7)

    eye = one_hot((128, 128), lambda o: o)

    def prompt_head(g, _):
        keys = kv[0, g].reshape(512, 128)
        values = kv[1, g].reshape(512, 128)
        rows = qy[:, :, :, g].astype(f32).reshape(512, 128).astype(bf16)
        scores = dot_t(keys, rows) * LOG2_SCALE
        mh, ml = in_two(jnp.max(scores, 0, keepdims=True))
        weights = jnp.exp2(scores - (mh + ml))
        stats = packed_stats(mh, ml, jnp.sum(weights, 0, keepdims=True))
        out = dot(dot_t(eye, values).astype(bf16), weights.astype(bf16)).astype(bf16)
        for dy in range(4):
            xs[dy, g, 0:128, :] = out[:, 128 * dy : 128 * dy + 128]
            xs[dy, g, 128:TALL, :] = stats[:, 128 * dy : 128 * dy + 128]
        return 0

    rs1 = []
    rs2 = []

    def over_y(k):
        arrived(rs1[k])
        first, n = tile_of(STARTS[k]), SIZES[k]
        for i in range(n):
            g = STARTS[k] + i
            out, top, total = merged([xs[0, g]] + [r1[dy, g] for dy in range(1, 4)])
            mh, ml = in_two(top)
            adjust = jnp.exp2(top - (mh + ml))
            ys[:, first + i] = dot_t(eye, (out * adjust).astype(bf16)).astype(bf16).reshape(16, 8, 128)
            sx[TAILS.index(LAST[k]), 16 * g : 16 * g + 8, :] = packed_stats(mh, ml, total * adjust)
        if k in TAILS:
            stats = dot_t(eye, sx[TAILS.index(k)]).astype(bf16)
            ys[:, first + n] = stats.reshape(16, 8, 128)
            n += 1
        t = pl.ds(first, n)
        rs2.append(new_group(r2.at[1:16, t]))
        for dz in (4, 3, 5, 2, 6, 1, 7, 0):
            for e in (0, 1):
                if dz or e:
                    send(rs2[k], ys.at[2 * dz + e, t], r2.at[2 * dz + e, t], dz=8 - dz, e=e)

    def prompt(k):
        arrived(q2[k])
        kv_arrived(k)
        lax.fori_loop(STARTS[k], STARTS[k] + SIZES[k], prompt_head, 0)
        h = heads_of(k)
        rs1.append(new_group(r1.at[1:4, h]))
        for dy in (2, 1, 3):
            send(rs1[k], xs.at[dy, h], r1.at[dy, h], dy=4 - dy)

    prompt(0)
    forward_kv(4)
    prompt(1)
    prompt(2)
    forward_kv(5)
    prompt(3)
    over_y(0)
    forward_kv(6)
    prompt(4)
    over_y(1)
    forward_kv(7)
    prompt(5)
    over_y(2)
    prompt(6)
    over_y(3)
    prompt(7)
    for k in range(4, CHUNKS):
        over_y(k)
    suffix(5, 16384 // PIECE)

    begun = 0
    for tail in TAILS:
        mine = range(begun, tail + 1)
        begun = tail + 1
        for k in mine:
            arrived(rs2[k])
        heads = range(STARTS[mine[0]], STARTS[tail] + SIZES[tail])
        at_stats = tile_of(heads[-1]) + 1
        for e in (0, 1):
            blocks = [r2.at[2 * dz + e] if dz or e else ys.at[0] for dz in range(8)]
            lane = iota((8, 128), 1)
            top_own = total_own = jnp.zeros((8, 128), f32)
            for g in heads:
                at = (e * 8 + g) * 8
                top_own = jnp.where(lane // 16 == g, sm[at : at + 8, :], top_own)
                total_own = jnp.where(lane // 16 == g, sl[at : at + 8, :], total_own)
            tiles = [b[at_stats].astype(f32) for b in blocks]
            tops = [t + pltpu.roll(t, 127, 1) for t in tiles] + [top_own]
            totals = [pltpu.roll(t, 126, 1) + pltpu.roll(t, 125, 1) for t in tiles] + [total_own]
            top = functools.reduce(jnp.maximum, tops)
            factors = [jnp.exp2(t - top) for t in tops]
            whole = functools.reduce(jnp.add, [f * t for f, t in zip(factors, totals)])
            factors = [f / whole for f in factors]
            for g in heads:
                at = (e * 8 + g) * 8
                parts = [b[tile_of(g)].astype(f32) for b in blocks] + [so[at : at + 8, :]]
                so[at : at + 8, :] = functools.reduce(
                    jnp.add, [p * f[:, 16 * g : 16 * g + 1] for p, f in zip(parts, factors)]
                )

    def final_row(o):
        j, g, r = o // 32, (o // 2) % 16, o % 2
        return (g // 8 + c) % 2 * 64 + g % 8 * 8 + j * 2 + r

    out_ref[...] = dot(one_hot((128, 128), final_row), so[...].astype(bf16)).astype(bf16)
    sent = sum(math.prod(arrivals.shape) for arrivals in groups)
    wait_for(send_sem, sk.at[0 : sent // 128])


def body(queries, prefix_keys, prefix_values, suffix_keys, suffix_values, lengths):
    vmem, anyspace = pltpu.VMEM, pl.BlockSpec(memory_space=pltpu.HBM)
    out = pl.pallas_call(
        kernel,
        name="attend",
        out_shape=jax.ShapeDtypeStruct((128, 128), bf16),
        in_specs=[anyspace] * 6,
        out_specs=pl.BlockSpec(memory_space=vmem),
        scratch_shapes=[
            vmem((128, 128), bf16),
            vmem((2, 1024, 128), bf16),
            vmem((16384, 128), bf16),
            vmem((16384, 128), bf16),
            vmem((2, HEADS, 8, 64, 128), bf16),
            vmem((2, HEADS, 64, 128), bf16),
            vmem((4, 8, 2, HEADS, 8, 128), bf16),
            vmem((HEADS, 8, 128), bf16),
            vmem((128, 128), bf16),
            vmem((4, HEADS, TALL, 128), bf16),
            vmem((4, HEADS, TALL, 128), bf16),
            vmem((len(TAILS), 128, 128), bf16),
            vmem((16, TILES, 8, 128), bf16),
            vmem((16, TILES, 8, 128), bf16),
            vmem((128, 128), f32),
            vmem((128, 128), f32),
            vmem((128, 128), f32),
            pltpu.SMEM((1,), jnp.int32),
            pltpu.SemaphoreType.DMA((6,)),
            pltpu.SemaphoreType.DMA,
            pltpu.SemaphoreType.DMA((SEMS + CHUNKS,)),
        ],
        compiler_params=pltpu.CompilerParams(
            collective_id=0, has_side_effects=True, vmem_limit_bytes=67_043_328
        ),
    )(
        lengths,
        queries.reshape(128, 128),
        prefix_keys.reshape(1024, 128),
        prefix_values.reshape(1024, 128),
        suffix_keys.reshape(16384, 128),
        suffix_values.reshape(16384, 128),
    )
    return out.reshape(1, 4, 32, 128)


def solution(mesh):
    return jax.shard_map(
        body,
        mesh=mesh,
        in_specs=(
            P(("kv", "batch"), None, None, None),
            P(("kv", "batch"), None, None),
            P(("kv", "batch"), None, None),
            P(("kv", "batch"), None, None, None),
            P(("kv", "batch"), None, None, None),
            P(("kv", "batch")),
        ),
        out_specs=P(("kv", "batch"), None, None, None),
        check_vma=False,
    )
```
